512 devices in a mesh: rows: 128 (over x, z, core), grp: 4 (over y).
Axes of the slice: x: 4, y: 4, z: 16, core: 2. Of those that a mesh axis runs over, the one named last changes fastest.
Arguments:
- operator: float32 [24576, 24576], P('rows', 'grp')
- block_inverse: float32 [3072, 24, 24], P('rows')
- block_len: int32 [128, 24], P('rows'), may hold values from 1 to 24, 192 in all within a row
- iterate: float32 [6, 24576], P(None, 'rows'), may hold values from -6 to 6
- residual: float32 [6, 24576], P(None, 'rows')
Outputs:
- new_iterate: float32 [6, 24576], P(None, 'rows')
- new_residual: float32 [6, 24576], P(None, 'rows')
The draws below stay inside these ranges and needn't reach their ends.
Inputs may be any that keep to these rules, and one draw needn't show every extreme that they name: Each row of block_len sums to 192.
All inputs are finite; a program needn't handle non-finite values.
Results may differ from the reference program's by a relative error of at most 0.0003.
Values sent between devices are 32-bit elements; how exact they have to be, the bound alone decides.
No kernel may reach another device: no remote copies, remote signals or barrier semaphores. Data moves between devices by JAX's collectives and lax.ppermute only.
A program may use at most 64 MiB of HBM per device.

```python
import math
import jax
import jax.numpy as jnp
import numpy as np
from jax import lax

BLOCK = 24
UNK_DEV = 192
SYSTEMS = 6
BLOCKS_DEV = 24
ORDER = 24576
N_ROWS = 128


def draw_operator(key, part):
    spread = 0.2 / math.sqrt(ORDER)
    entries = jax.random.normal(key, (ORDER, ORDER), jnp.float32) * spread
    diag_index = jnp.arange(ORDER)
    return entries.at[diag_index, diag_index].add(1.0)


def draw_block_inverse(key, part):
    counted = N_ROWS * BLOCKS_DEV
    subkeys = jax.random.split(jax.random.fold_in(key, 11), 2)
    diagonal = jax.random.uniform(subkeys[0], (counted, BLOCK), jnp.float32, 0.9, 1.25)
    spread = 0.1 / math.sqrt(BLOCK)
    noise = jax.random.normal(subkeys[1], (counted, BLOCK, BLOCK), jnp.float32) * spread
    return noise + diagonal[:, :, None] * jnp.eye(BLOCK, dtype=jnp.float32)[None, :, :]


def draw_residual(key, part):
    subkeys = jax.random.split(jax.random.fold_in(key, 23), 1)
    growth = jnp.exp(jnp.log(3.0) * jnp.arange(ORDER, dtype=jnp.float32) / ORDER)
    values = jax.random.normal(subkeys[0], (SYSTEMS, ORDER), jnp.float32)
    return values * growth[None, :]


def level_of(key, dims, shards, least, top_value):
    def one(position, blocks):
        draws = jax.random.uniform(jax.random.fold_in(jax.random.fold_in(key, 6), position), (blocks,), jnp.float32, least / len(shards), top_value / len(shards))
        return jnp.repeat(jnp.exp(draws), dims[position] // blocks).reshape((-1,) + (1,) * (len(dims) - position - 1))

    gain = one(*shards[0])
    for cut in shards[1:]:
        gain = gain * one(*cut)
    return gain


def split_up(number_of, total, reach, lean):
    portions = [(1 << 20) // math.isqrt(grade ** lean) + 1 for grade in range(2, number_of + 1)]
    surplus, given = total - reach - (number_of - 1), [1] * (number_of - 1)
    while surplus > 0:
        movable = [i for i in range(number_of - 1) if given[i] < reach]
        mass, left = sum([portions[i] for i in movable]), surplus
        for i in movable:
            more = min(reach - given[i], max(1, left * portions[i] // mass), surplus)
            given[i] = given[i] + more
            surplus = surplus - more
    return np.array([reach] + given)


def ragged_sizes(own_key, amount, total, limit, lean):
    if amount == 2:
        one = jax.random.randint(own_key, (), max(1, total - limit), min(limit, total - 1) + 1)
        return jnp.stack([one, total - one])
    tallies = jnp.asarray(split_up(amount, total, limit, lean), jnp.int32)
    couples = (amount - 1) // 2
    source_of, taker = tallies[1:1 + 2 * couples:2], tallies[2:2 + 2 * couples:2]
    slack = jnp.minimum(source_of - 1, limit - taker)
    passed = jax.random.randint(jax.random.fold_in(own_key, 1), (couples,), 0, 1 << 20) % (slack + 1)
    tallies = tallies.at[1:1 + 2 * couples:2].set(source_of - passed).at[2:2 + 2 * couples:2].set(taker + passed)
    return tallies[jax.random.permutation(jax.random.fold_in(own_key, 2), amount)]


def gaussian(stream_key, shape, deviation, limit, cuts=(), kind=jnp.bfloat16):
    array = jax.random.normal(stream_key, shape, jnp.float32) * deviation
    if len(cuts) > 0:
        array = level_of(stream_key, shape, cuts, -0.22, 0.18) * array
    return jnp.clip(array, min=-limit, max=limit).astype(kind)


def setup_inputs(seed: int = 0) -> dict:
    key_of = jax.random.split(jax.random.key(seed), 6)
    return {
        "operator": draw_operator(jax.random.fold_in(key_of[5], 71), 0),
        "block_inverse": draw_block_inverse(jax.random.fold_in(key_of[5], 71), 0),
        "block_len": jax.vmap(lambda own: ragged_sizes(own, BLOCKS_DEV, UNK_DEV, BLOCK, 2))(jax.random.split(key_of[2], N_ROWS)).reshape((N_ROWS, BLOCKS_DEV)).astype(jnp.int32),
        "iterate": gaussian(key_of[3], (SYSTEMS, ORDER), 1.0, 6.0, ((1, 128),), jnp.float32),
        "residual": draw_residual(jax.random.fold_in(key_of[5], 71), 0),
    }


highest = lax.Precision.HIGHEST


def block_apply(lengths, inverse, vector):
    width = vector.shape[1]
    starts = jnp.cumsum(lengths) - lengths
    offset = jnp.arange(BLOCK, dtype=jnp.int32)
    column = jnp.arange(width, dtype=jnp.int32)
    select = ((column[None, None, :] == starts[:, None, None] + offset[None, :, None])
              & (offset[None, :, None] < lengths[:, None, None])).astype(jnp.float32)
    pieces = jnp.einsum('bku,ru->rbk', select, vector, precision=highest)
    solved = jnp.einsum('bkl,rbl->rbk', inverse, pieces, precision=highest)
    return jnp.einsum('bku,rbk->ru', select, solved, precision=highest)


def precondition(block_len, block_inverse, vector):
    groups = block_len.shape[0]
    stacked = block_inverse.reshape(groups, block_len.shape[1], BLOCK, BLOCK)
    pieces = vector.reshape(vector.shape[0], groups, -1).transpose(1, 0, 2)
    result = lax.map(lambda element: block_apply(element[0], element[1], element[2]),
                     (block_len, stacked, pieces))
    return result.transpose(1, 0, 2).reshape(vector.shape)


def product(operator, vector):
    return jnp.dot(vector, operator, precision=highest)


def reference(operator, block_inverse, block_len, iterate, residual):
    lifted = precondition(block_len, block_inverse, residual)
    mapped = product(operator, lifted)
    norm_res = jnp.sum(residual * residual, axis=1)
    curve_one = jnp.sum(residual * mapped, axis=1)
    alpha_step = norm_res / curve_one
    middle = residual - alpha_step[:, None] * mapped
    lifted_mid = precondition(block_len, block_inverse, middle)
    mapped_mid = product(operator, lifted_mid)
    cross_mid = jnp.sum(mapped_mid * middle, axis=1)
    square_mid = jnp.sum(mapped_mid * mapped_mid, axis=1)
    omega_step = cross_mid / square_mid
    new_iterate = iterate + alpha_step[:, None] * lifted + omega_step[:, None] * lifted_mid
    new_residual = middle - omega_step[:, None] * mapped_mid
    return new_iterate, new_residual
```

```python
import jax
import jax.numpy as jnp
from jax import lax
from jax.sharding import Mesh
from jax.sharding import PartitionSpec as P

ROWS = ("x", "z", "c")

highest = lax.Precision.HIGHEST


def exchanged(pieces, axes):
    return lax.all_to_all(pieces, axes, split_axis=0, concat_axis=0, tiled=True)


def selection(lengths, width, depth):
    starts = jnp.cumsum(lengths) - lengths
    offset = jnp.arange(depth, dtype=jnp.int32)
    column = jnp.arange(width, dtype=jnp.int32)
    return (
        (column[None, None, :] == starts[:, None, None] + offset[None, :, None])
        & (offset[None, :, None] < lengths[:, None, None])
    ).astype(jnp.float32)


def block_apply(select, inverse, vector):
    pieces = jnp.einsum("bku,ru->rbk", select, vector, precision=highest)
    solved = jnp.einsum("bkl,rbl->rbk", inverse, pieces, precision=highest)
    return jnp.einsum("bku,rbk->ru", select, solved, precision=highest)


def body(operator, block_inverse, block_len, iterate, residual):
    nx, nz, nc, ny = (lax.axis_size(a) for a in ("x", "z", "c", "y"))
    systems, unknowns = residual.shape
    pair = -(-systems // nx)
    spare = pair * nx - systems
    select = selection(block_len[0], unknowns, block_inverse.shape[1])
    my_x = lax.axis_index("x")

    def pairs(rows):
        return jnp.pad(rows, ((0, spare), (0, 0))).reshape(nx, pair * unknowns)

    def reduced(vector):
        partial_value = jnp.dot(vector, operator, precision=highest)
        padded = jnp.pad(partial_value, ((0, spare), (0, 0)))
        cut = padded.reshape(nx, pair, nz, nc, unknowns).transpose(0, 3, 2, 1, 4)
        cut = cut.reshape(nx * nc, nz, pair * unknowns)
        near = exchanged(cut, ("x", "c")).sum(axis=0)
        far = exchanged(near[:, None, :], "z")
        return far.sum(axis=(0, 1))

    def delivered(pieces):
        arrived = exchanged(pieces.reshape(nx * ny, 1, -1), ("x", "y")).reshape(nx, ny, -1)
        return arrived

    def mine(arrived):
        row = lax.dynamic_index_in_dim(arrived, my_x, 1, keepdims=False)
        return row.reshape(nx * pair, unknowns)[:systems]

    width = pair * unknowns
    lifted = block_apply(select, block_inverse, residual)
    piece = reduced(lifted)
    sent = jnp.concatenate(
        [jnp.broadcast_to(piece, (nx, ny, width)), jnp.broadcast_to(pairs(residual)[:, None], (nx, ny, width))],
        axis=2,
    )
    arrived = delivered(sent)
    mapped = mine(arrived[:, :, :width])
    my_y = lax.axis_index("y")
    other = lax.dynamic_index_in_dim(arrived[:, 0, width:], my_y, 0, keepdims=False)
    lifted_two = block_apply(select, block_inverse, mapped)
    piece_two = reduced(lifted_two)

    r, m, t = (v.reshape(pair, unknowns) for v in (other, piece, piece_two))
    dots = jnp.stack([jnp.sum(a * b, axis=1) for a, b in ((r, r), (r, m), (m, m), (t, r), (t, m), (t, t))])
    tail = jnp.pad(dots.reshape(-1), (0, 128 - dots.size))
    arrived = delivered(jnp.broadcast_to(jnp.concatenate([piece_two, tail]), (nx, ny, width + 128)))
    mapped_two = mine(arrived[:, :, :width])
    near = arrived[:, :, width : width + dots.size].sum(axis=1).reshape(-1)
    totals = exchanged(jnp.broadcast_to(near, (nz * nc, 1, near.size)), ("z", "c")).sum(axis=(0, 1))
    totals = totals.reshape(nx, 6, pair).transpose(1, 0, 2).reshape(6, nx * pair)[:, :systems]
    norm_res, curve_one, square_map, mixed_res, mixed_map, square_two = totals

    alpha_step = norm_res / curve_one
    cross_mid = (
        curve_one
        - alpha_step * square_map
        - alpha_step * mixed_res
        + alpha_step * alpha_step * mixed_map
    )
    square_mid = square_map - 2.0 * alpha_step * mixed_map + alpha_step * alpha_step * square_two
    omega_step = cross_mid / square_mid
    middle = residual - alpha_step[:, None] * mapped
    lifted_mid = lifted - alpha_step[:, None] * lifted_two
    mapped_mid = mapped - alpha_step[:, None] * mapped_two
    new_iterate = iterate + alpha_step[:, None] * lifted + omega_step[:, None] * lifted_mid
    new_residual = middle - omega_step[:, None] * mapped_mid
    return (new_iterate, new_residual)


def solution(mesh):
    torus = Mesh(mesh.devices.reshape(4, 16, 2, mesh.shape["grp"]), ("x", "z", "c", "y"))
    placed = (P(ROWS, "y"), P(ROWS, None, None), P(ROWS, None), P(None, ROWS), P(None, ROWS))
    return jax.shard_map(
        body, mesh=torus, in_specs=placed, out_specs=(P(None, ROWS), P(None, ROWS)), check_vma=False
    )
```

```python
import functools

import jax
import jax.numpy as jnp
from jax import lax
from jax.experimental import pallas as pl
from jax.experimental.pallas import tpu as pltpu
from jax.sharding import Mesh
from jax.sharding import PartitionSpec as P

ROWS = ("x", "z", "c")
NX, NZ, NC, NY = 4, 16, 2, 4
SYS, UNK, LANE = 6, 192, 128
REST = UNK - LANE
PAIR = 2
WIDE = PAIR * UNK
TILES = WIDE // LANE
BLOCKS = 24
COPIES = 4
DOTS = 6

highest = lax.Precision.HIGHEST
f32 = jnp.float32
VM = pl.BlockSpec(memory_space=pltpu.VMEM)


def iota(shape, dim):
    return lax.broadcasted_iota(jnp.int32, shape, dim)


def nt(a, b):
    return lax.dot_general(a, b, (((1,), (1,)), ((), ())), precision=highest, preferred_element_type=f32)


def preconditioner(len_ref, inverse):
    slots = BLOCKS * BLOCKS
    slot = iota((1, slots), 1)
    block = slot // BLOCKS
    within = slot - block * BLOCKS
    column = iota((1, UNK), 1)
    target = jnp.full((1, slots), -1, jnp.int32)
    first = jnp.zeros((1, UNK), jnp.int32)
    last = jnp.zeros((1, UNK), jnp.int32)
    start = jnp.int32(0)
    for b in range(BLOCKS):
        size = len_ref[0, b]
        end = start + size
        target = jnp.where((block == b) & (within < size), start + within, target)
        inside = (column >= start) & (column < end)
        first = jnp.where(inside, start, first)
        last = jnp.where(inside, end, last)
        start = end
    pick = (iota((UNK, slots), 0) == target).astype(f32)
    rows = jnp.dot(pick, inverse, precision=highest, preferred_element_type=f32)
    spread = (iota((BLOCKS, UNK), 0) == column - first).astype(f32)
    full = jnp.dot(rows, spread, precision=highest, preferred_element_type=f32)
    row = iota((UNK, UNK), 0)
    return jnp.where((row >= first) & (row < last), full, 0.0)


def encoded(vector, core):
    main = jnp.where(core == 0, vector[:, :LANE], vector[:, REST:])
    rest = jnp.where(core == 0, vector[:, LANE:], vector[:, :REST])
    rows = []
    for p in range(SYS // PAIR):
        a, b = PAIR * p, PAIR * p + 1
        rows.append(jnp.concatenate([main[a : a + 1], main[b : b + 1], rest[a : a + 1], rest[b : b + 1]], axis=1))
    return rows


def decoded(rows, core):
    main = jnp.concatenate([r[:, k * LANE : (k + 1) * LANE] for r in rows for k in range(PAIR)], axis=0)
    rest = jnp.concatenate(
        [r[:, PAIR * LANE + k * REST : PAIR * LANE + (k + 1) * REST] for r in rows for k in range(PAIR)], axis=0
    )
    return jnp.where(
        core == 0, jnp.concatenate([main, rest], axis=1), jnp.concatenate([rest, main], axis=1)
    )


def copies_of(operator_ref, held, sems):
    width = operator_ref.shape[1] // COPIES
    return [
        pltpu.make_async_copy(
            operator_ref.at[:, k * width : (k + 1) * width], held.at[:, k * width : (k + 1) * width], sems.at[k]
        )
        for k in range(COPIES)
    ]


def product(matrix, vector, copies, held, spread, cut_ref):
    turned = nt(matrix, vector)
    for s in range(SYS):
        spread[s] = jnp.broadcast_to(turned[:, s : s + 1], (UNK, LANE))
    for k in range(SYS // PAIR, NX):
        for c in range(NC):
            cut_ref[k * NC + c] = jnp.zeros((NZ, 1, WIDE), f32)
    low = iota((1, LANE), 1) < REST

    def one(z, carry):
        base = pl.multiple_of(z * (NC * UNK), LANE)
        totals = [[None] * TILES for _ in range(SYS)]
        for j in range(UNK // 8):
            tiles = [held[8 * j : 8 * j + 8, pl.ds(base + k * LANE, LANE)] for k in range(TILES)]
            for s in range(SYS):
                v = spread[s, 8 * j : 8 * j + 8, :]
                for k in range(TILES):
                    term = tiles[k] * v
                    totals[s][k] = term if j == 0 else totals[s][k] + term
        sums = [[jnp.sum(totals[s][k], axis=0, keepdims=True) for k in range(TILES)] for s in range(SYS)]
        for p in range(SYS // PAIR):
            a, b = sums[PAIR * p], sums[PAIR * p + 1]
            lo = jnp.where(low, a[1], pltpu.roll(b[1], REST, 1))
            hi = jnp.where(low, pltpu.roll(a[1], REST, 1), b[1])
            for c, row in ((0, (a[0], b[0], lo)), (1, (a[2], b[2], hi))):
                for k in range(TILES):
                    cut_ref[NC * p + c, z, :, k * LANE : (k + 1) * LANE] = row[k]
        return carry

    per = NZ // COPIES
    for k in range(COPIES):
        copies[k].wait()
        lax.fori_loop(k * per, (k + 1) * per, one, 0)


def first_kernel(
    len_hbm, inverse_hbm, residual_hbm, iterate_hbm, operator_hbm,
    cut_ref, matrix_ref, lifted_ref, ride_ref, residual_ref, iterate_ref,
    held, spread, sems, lengths, inverse, small_sems,
):
    small = [
        pltpu.make_async_copy(source, target, small_sems.at[k])
        for k, (source, target) in enumerate(
            ((len_hbm, lengths), (inverse_hbm, inverse), (residual_hbm, residual_ref), (iterate_hbm, iterate_ref))
        )
    ]
    for copy in small:
        copy.start()
    copies = copies_of(operator_hbm, held, sems)
    for copy in copies:
        copy.start()
    for copy in small:
        copy.wait()
    core = lax.axis_index("c")
    residual = residual_ref[...]
    matrix = preconditioner(lengths, inverse[...])
    product(matrix, residual, copies, held, spread, cut_ref)
    matrix_ref[...] = matrix
    lifted_ref[...] = nt(residual, matrix)
    rows = encoded(residual, core)
    for x in range(NX):
        row = rows[x] if x < len(rows) else jnp.zeros((1, WIDE), f32)
        for y in range(NY):
            ride_ref[x * NY + y] = row


def second_kernel(
    arrived_ref, matrix_ref, operator_hbm, cut_ref, mapped_ref, lifted_ref, piece_ref, other_ref, held, spread, sems
):
    copies = copies_of(operator_hbm, held, sems)
    for copy in copies:
        copy.start()
    core, x, y = lax.axis_index("c"), lax.axis_index("x"), lax.axis_index("y")
    mapped = decoded([arrived_ref[p * NY + x][:, :WIDE] for p in range(SYS // PAIR)], core)
    matrix = matrix_ref[...]
    product(matrix, mapped, copies, held, spread, cut_ref)
    mapped_ref[...] = mapped
    lifted_ref[...] = nt(mapped, matrix)
    piece_ref[...] = arrived_ref[x * NY + y][:, :WIDE]
    other_ref[...] = arrived_ref[y * NY][:, WIDE:]


def dots_kernel(far_ref, piece_ref, other_ref, sent_ref):
    t = jnp.sum(far_ref[...], axis=0)
    m, r = piece_ref[...], other_ref[...]
    terms = jnp.concatenate([r * r, r * m, m * m, t * r, t * m, t * t], axis=0)
    shared = terms[:, PAIR * LANE :]
    low = iota(shared.shape, 1) < REST
    sides = jnp.concatenate(
        [terms[:, :LANE] + jnp.where(low, shared, 0.0), terms[:, LANE : 2 * LANE] + jnp.where(low, 0.0, shared)], axis=0
    )
    column = jnp.sum(sides, axis=1, keepdims=True)
    shape = (PAIR * DOTS, LANE)
    line = jnp.sum(jnp.where(iota(shape, 0) == iota(shape, 1), column, 0.0), axis=0, keepdims=True)
    row = jnp.concatenate([t, line], axis=1)
    for k in range(NX * NY):
        sent_ref[k] = row


def near_kernel(arrived_ref, sent_ref):
    total = None
    for x in range(NX):
        line = None
        for y in range(NY):
            part = arrived_ref[x * NY + y][:, WIDE:]
            line = part if line is None else line + part
        if x:
            line = pltpu.roll(line, x * PAIR * DOTS, 1)
        total = line if total is None else total + line
    for k in range(NZ * NC):
        sent_ref[k] = total


def last_kernel(far_ref, arrived_ref, iterate_ref, residual_ref, mapped_ref, lifted_ref, lifted_two_ref, new_iterate_ref, new_residual_ref):
    core, x = lax.axis_index("c"), lax.axis_index("x")
    totals = jnp.sum(far_ref[...], axis=0)
    lane = iota((SYS, LANE), 1)
    system = iota((SYS, LANE), 0)
    home = (system // PAIR) * (PAIR * DOTS) + (system % PAIR) * DOTS
    norm_res, curve_one, square_map, mixed_res, mixed_map, square_two = (
        jnp.sum(jnp.where(lane == home + d, totals, 0.0), axis=1, keepdims=True) for d in range(DOTS)
    )
    alpha = norm_res / curve_one
    cross_mid = curve_one - alpha * square_map - alpha * mixed_res + alpha * alpha * mixed_map
    square_mid = square_map - 2.0 * alpha * mixed_map + alpha * alpha * square_two
    omega = cross_mid / square_mid
    mapped, lifted = mapped_ref[...], lifted_ref[...]
    mapped_two = decoded([arrived_ref[p * NY + x][:, :WIDE] for p in range(SYS // PAIR)], core)
    middle = residual_ref[...] - alpha * mapped
    lifted_mid = lifted - alpha * lifted_two_ref[...]
    new_iterate_ref[...] = iterate_ref[...] + alpha * lifted + omega * lifted_mid
    new_residual_ref[...] = middle - omega * (mapped - alpha * mapped_two)


def exchanged(pieces, axes):
    return lax.all_to_all(pieces, axes, split_axis=0, concat_axis=0, tiled=True)


def body(operator, block_inverse, block_len, iterate, residual):
    def shape(*lengths):
        return jax.ShapeDtypeStruct(lengths, f32)

    hbm = pl.BlockSpec(memory_space=pltpu.HBM)
    cut_shape = shape(NX * NC, NZ, 1, WIDE)
    small = shape(SYS, UNK)
    row = shape(1, WIDE)
    scratch = [
        pltpu.VMEM(operator.shape, f32),
        pltpu.VMEM((SYS, UNK, LANE), f32),
        pltpu.SemaphoreType.DMA((COPIES,)),
    ]
    params = pltpu.CompilerParams(vmem_limit_bytes=16 << 20)
    light = pltpu.CompilerParams(vmem_limit_bytes=4 << 20)
    inputs = (block_len, block_inverse.reshape(BLOCKS * BLOCKS, BLOCKS), residual, iterate, operator)
    inputs = [pltpu.with_memory_space_constraint(a, pltpu.HBM) for a in inputs]

    cut, matrix, lifted, ride, residual, iterate = pl.pallas_call(
        first_kernel,
        out_shape=(cut_shape, shape(UNK, UNK), small, shape(NX * NY, 1, WIDE), small, small),
        in_specs=[hbm] * 5,
        out_specs=[VM] * 6,
        scratch_shapes=scratch
        + [
            pltpu.SMEM((1, BLOCKS), jnp.int32),
            pltpu.VMEM((BLOCKS * BLOCKS, BLOCKS), f32),
            pltpu.SemaphoreType.DMA((4,)),
        ],
        compiler_params=params,
        name="first_product",
    )(*inputs)

    def reduced(cut):
        near = exchanged(cut, ("x", "c")).sum(axis=0)
        return exchanged(near, "z")

    piece = reduced(cut).sum(axis=0)
    sent = jnp.concatenate([jnp.broadcast_to(piece[None], ride.shape), ride], axis=2)
    arrived = exchanged(sent, ("x", "y"))

    cut, mapped, lifted_two, piece, other = pl.pallas_call(
        second_kernel,
        out_shape=(cut_shape, small, small, row, row),
        in_specs=[VM, VM, hbm],
        out_specs=[VM] * 5,
        scratch_shapes=scratch,
        compiler_params=params,
        name="second_product",
    )(arrived, matrix, inputs[4])

    sent = pl.pallas_call(
        dots_kernel,
        out_shape=shape(NX * NY, 1, WIDE + LANE),
        in_specs=[VM] * 3,
        out_specs=VM,
        compiler_params=light,
        name="dots",
    )(reduced(cut), piece, other)
    arrived = exchanged(sent, ("x", "y"))
    sent = pl.pallas_call(
        near_kernel,
        out_shape=shape(NZ * NC, 1, LANE),
        in_specs=[VM],
        out_specs=VM,
        compiler_params=light,
        name="near_dots",
    )(arrived)
    far = exchanged(sent, ("z", "c"))
    return tuple(
        pl.pallas_call(
            last_kernel,
            out_shape=(small, small),
            in_specs=[VM] * 7,
            out_specs=[VM] * 2,
            compiler_params=light,
            name="update",
        )(far, arrived, iterate, residual, mapped, lifted, lifted_two)
    )


def solution(mesh):
    torus = Mesh(mesh.devices.reshape(NX, NZ, NC, NY), ("x", "z", "c", "y"))
    placed = (P(ROWS, "y"), P(ROWS, None, None), P(ROWS, None), P(None, ROWS), P(None, ROWS))
    return jax.shard_map(
        body, mesh=torus, in_specs=placed, out_specs=(P(None, ROWS), P(None, ROWS)), check_vma=False
    )
```

```python
import functools

import jax
import jax.numpy as jnp
from jax import lax
from jax.experimental import pallas as pl
from jax.experimental.pallas import tpu as pltpu
from jax.sharding import Mesh
from jax.sharding import PartitionSpec as P

Z = ("zh", "zl")
ROWS = ("x", *Z, "c")
NX, NH, NL, NC, NY = 4, 8, 2, 2, 4
NZ = NH * NL
SYS, UNK, LANE = 6, 192, 128
REST = UNK - LANE
PAIR = 2
WIDE = PAIR * UNK
TILES = WIDE // LANE
BLOCKS = 24
COPIES = 4
DOTS = 6

highest = lax.Precision.HIGHEST
f32 = jnp.float32
VM = pl.BlockSpec(memory_space=pltpu.VMEM)


def iota(shape, dim):
    return lax.broadcasted_iota(jnp.int32, shape, dim)


def nt(a, b):
    return lax.dot_general(a, b, (((1,), (1,)), ((), ())), precision=highest, preferred_element_type=f32)


def preconditioner(len_ref, inverse):
    slots = BLOCKS * BLOCKS
    slot = iota((1, slots), 1)
    block = slot // BLOCKS
    within = slot - block * BLOCKS
    column = iota((1, UNK), 1)
    target = jnp.full((1, slots), -1, jnp.int32)
    first = jnp.zeros((1, UNK), jnp.int32)
    last = jnp.zeros((1, UNK), jnp.int32)
    start = jnp.int32(0)
    for b in range(BLOCKS):
        size = len_ref[0, b]
        end = start + size
        target = jnp.where((block == b) & (within < size), start + within, target)
        inside = (column >= start) & (column < end)
        first = jnp.where(inside, start, first)
        last = jnp.where(inside, end, last)
        start = end
    pick = (iota((UNK, slots), 0) == target).astype(f32)
    rows = jnp.dot(pick, inverse, precision=highest, preferred_element_type=f32)
    spread = (iota((BLOCKS, UNK), 0) == column - first).astype(f32)
    full = jnp.dot(rows, spread, precision=highest, preferred_element_type=f32)
    row = iota((UNK, UNK), 0)
    return jnp.where((row >= first) & (row < last), full, 0.0)


def encoded(vector, core):
    main = jnp.where(core == 0, vector[:, :LANE], vector[:, REST:])
    rest = jnp.where(core == 0, vector[:, LANE:], vector[:, :REST])
    rows = []
    for p in range(SYS // PAIR):
        a, b = PAIR * p, PAIR * p + 1
        rows.append(jnp.concatenate([main[a : a + 1], main[b : b + 1], rest[a : a + 1], rest[b : b + 1]], axis=1))
    return rows


def decoded(rows, core):
    main = jnp.concatenate([r[:, k * LANE : (k + 1) * LANE] for r in rows for k in range(PAIR)], axis=0)
    rest = jnp.concatenate(
        [r[:, PAIR * LANE + k * REST : PAIR * LANE + (k + 1) * REST] for r in rows for k in range(PAIR)], axis=0
    )
    return jnp.where(
        core == 0, jnp.concatenate([main, rest], axis=1), jnp.concatenate([rest, main], axis=1)
    )


def copies_of(operator_ref, held, sems):
    width = operator_ref.shape[1] // COPIES
    return [
        pltpu.make_async_copy(
            operator_ref.at[:, k * width : (k + 1) * width], held.at[:, k * width : (k + 1) * width], sems.at[k]
        )
        for k in range(COPIES)
    ]


def product(matrix, vector, copies, held, spread, cut_ref):
    steps = cut_ref.shape[1]
    inner = NZ // steps
    turned = nt(matrix, vector)
    for s in range(SYS):
        spread[s] = jnp.broadcast_to(turned[:, s : s + 1], (UNK, LANE))
    for k in range(SYS // PAIR * inner * NC, NX * inner * NC):
        cut_ref[k] = jnp.zeros((steps, 1, WIDE), f32)
    low = iota((1, LANE), 1) < REST

    def one(z, carry):
        base = pl.multiple_of(z * (NC * UNK), LANE)
        totals = [[None] * TILES for _ in range(SYS)]
        for j in range(UNK // 8):
            tiles = [held[8 * j : 8 * j + 8, pl.ds(base + k * LANE, LANE)] for k in range(TILES)]
            for s in range(SYS):
                v = spread[s, 8 * j : 8 * j + 8, :]
                for k in range(TILES):
                    term = tiles[k] * v
                    totals[s][k] = term if j == 0 else totals[s][k] + term
        sums = [[jnp.sum(totals[s][k], axis=0, keepdims=True) for k in range(TILES)] for s in range(SYS)]
        for p in range(SYS // PAIR):
            a, b = sums[PAIR * p], sums[PAIR * p + 1]
            lo = jnp.where(low, a[1], pltpu.roll(b[1], REST, 1))
            hi = jnp.where(low, pltpu.roll(a[1], REST, 1), b[1])
            for c, row in ((0, (a[0], b[0], lo)), (1, (a[2], b[2], hi))):
                for k in range(TILES):
                    home = (p * inner + lax.rem(z, inner)) * NC + c
                    cut_ref[home, lax.div(z, inner), :, k * LANE : (k + 1) * LANE] = row[k]
        return carry

    per = NZ // COPIES
    for k in range(COPIES):
        copies[k].wait()
        lax.fori_loop(k * per, (k + 1) * per, one, 0)


def first_kernel(
    len_hbm, inverse_hbm, residual_hbm, iterate_hbm, operator_hbm,
    cut_ref, matrix_ref, lifted_ref, ride_ref, residual_ref, iterate_ref,
    held, spread, sems, lengths, inverse, small_sems,
):
    small = [
        pltpu.make_async_copy(source, target, small_sems.at[k])
        for k, (source, target) in enumerate(
            ((len_hbm, lengths), (inverse_hbm, inverse), (residual_hbm, residual_ref), (iterate_hbm, iterate_ref))
        )
    ]
    for copy in small:
        copy.start()
    copies = copies_of(operator_hbm, held, sems)
    for copy in copies:
        copy.start()
    for copy in small:
        copy.wait()
    core = lax.axis_index("c")
    residual = residual_ref[...]
    matrix = preconditioner(lengths, inverse[...])
    product(matrix, residual, copies, held, spread, cut_ref)
    matrix_ref[...] = matrix
    lifted_ref[...] = nt(residual, matrix)
    rows = encoded(residual, core)
    for x in range(NX):
        row = rows[x] if x < len(rows) else jnp.zeros((1, WIDE), f32)
        for y in range(NY):
            ride_ref[x * NY + y] = row


def second_kernel(
    arrived_ref, matrix_ref, operator_hbm, cut_ref, mapped_ref, lifted_ref, piece_ref, other_ref, held, spread, sems
):
    copies = copies_of(operator_hbm, held, sems)
    for copy in copies:
        copy.start()
    core, x, y = lax.axis_index("c"), lax.axis_index("x"), lax.axis_index("y")
    mapped = decoded([arrived_ref[p * NY + x][:, :WIDE] for p in range(SYS // PAIR)], core)
    matrix = matrix_ref[...]
    product(matrix, mapped, copies, held, spread, cut_ref)
    mapped_ref[...] = mapped
    lifted_ref[...] = nt(mapped, matrix)
    piece_ref[...] = arrived_ref[x * NY + y][:, :WIDE]
    other_ref[...] = arrived_ref[y * NY][:, WIDE:]


def share_kernel(arrived_ref, piece_ref, other_ref, sent_ref):
    near = jnp.sum(arrived_ref[...], axis=0)
    for k in range(NH):
        sent_ref[k, :NH] = near
        sent_ref[k, NH] = piece_ref[...]
        sent_ref[k, NH + 1] = other_ref[...]


def dots_kernel(far_ref, sent_ref):
    mine = far_ref[0, lax.axis_index("zh")]
    for k in range(1, NH):
        mine = mine + far_ref[k, lax.axis_index("zh")]
    terms = [None] * DOTS
    for h in range(NH):
        t = far_ref[0, h]
        for k in range(1, NH):
            t = t + far_ref[k, h]
        m, r = far_ref[h, NH], far_ref[h, NH + 1]
        for d, term in enumerate((r * r, r * m, m * m, t * r, t * m, t * t)):
            terms[d] = term if h == 0 else terms[d] + term
    terms = jnp.concatenate(terms, axis=0)
    shared = terms[:, PAIR * LANE :]
    low = iota(shared.shape, 1) < REST
    sides = jnp.concatenate(
        [terms[:, :LANE] + jnp.where(low, shared, 0.0), terms[:, LANE : 2 * LANE] + jnp.where(low, 0.0, shared)], axis=0
    )
    column = jnp.sum(sides, axis=1, keepdims=True)
    shape = (PAIR * DOTS, LANE)
    line = jnp.sum(jnp.where(iota(shape, 0) == iota(shape, 1), column, 0.0), axis=0, keepdims=True)
    row = jnp.concatenate([mine, line], axis=1)
    for k in range(sent_ref.shape[0]):
        sent_ref[k] = row


def last_kernel(arrived_ref, iterate_ref, residual_ref, mapped_ref, lifted_ref, lifted_two_ref, new_iterate_ref, new_residual_ref):
    core, x, low = lax.axis_index("c"), lax.axis_index("x"), lax.axis_index("zl")
    group = NL * NC * NY
    totals = None
    for k in range(NX):
        line = jnp.sum(arrived_ref[k * group : (k + 1) * group, :, WIDE:], axis=0)
        if k:
            line = pltpu.roll(line, k * PAIR * DOTS, 1)
        totals = line if totals is None else totals + line
    lane = iota((SYS, LANE), 1)
    system = iota((SYS, LANE), 0)
    home = (system // PAIR) * (PAIR * DOTS) + (system % PAIR) * DOTS
    norm_res, curve_one, square_map, mixed_res, mixed_map, square_two = (
        jnp.sum(jnp.where(lane == home + d, totals, 0.0), axis=1, keepdims=True) for d in range(DOTS)
    )
    alpha = norm_res / curve_one
    cross_mid = curve_one - alpha * square_map - alpha * mixed_res + alpha * alpha * mixed_map
    square_mid = square_map - 2.0 * alpha * mixed_map + alpha * alpha * square_two
    omega = cross_mid / square_mid
    mapped, lifted = mapped_ref[...], lifted_ref[...]
    home = (low * NC + core) * NY + x
    mapped_two = decoded([arrived_ref[p * group + home][:, :WIDE] for p in range(SYS // PAIR)], core)
    middle = residual_ref[...] - alpha * mapped
    lifted_mid = lifted - alpha * lifted_two_ref[...]
    new_iterate_ref[...] = iterate_ref[...] + alpha * lifted + omega * lifted_mid
    new_residual_ref[...] = middle - omega * (mapped - alpha * mapped_two)


def exchanged(pieces, axes):
    return lax.all_to_all(pieces, axes, split_axis=0, concat_axis=0, tiled=True)


def body(operator, block_inverse, block_len, iterate, residual):
    def shape(*lengths):
        return jax.ShapeDtypeStruct(lengths, f32)

    hbm = pl.BlockSpec(memory_space=pltpu.HBM)
    small = shape(SYS, UNK)
    row = shape(1, WIDE)
    scratch = [
        pltpu.VMEM(operator.shape, f32),
        pltpu.VMEM((SYS, UNK, LANE), f32),
        pltpu.SemaphoreType.DMA((COPIES,)),
    ]
    params = pltpu.CompilerParams(vmem_limit_bytes=16 << 20)
    light = pltpu.CompilerParams(vmem_limit_bytes=4 << 20)
    inputs = (block_len, block_inverse.reshape(BLOCKS * BLOCKS, BLOCKS), residual, iterate, operator)
    inputs = [pltpu.with_memory_space_constraint(a, pltpu.HBM) for a in inputs]

    cut, matrix, lifted, ride, residual, iterate = pl.pallas_call(
        first_kernel,
        out_shape=(shape(NX * NC, NZ, 1, WIDE), shape(UNK, UNK), small, shape(NX * NY, 1, WIDE), small, small),
        in_specs=[hbm] * 5,
        out_specs=[VM] * 6,
        scratch_shapes=scratch
        + [
            pltpu.SMEM((1, BLOCKS), jnp.int32),
            pltpu.VMEM((BLOCKS * BLOCKS, BLOCKS), f32),
            pltpu.SemaphoreType.DMA((4,)),
        ],
        compiler_params=params,
        name="first_product",
    )(*inputs)

    near = exchanged(cut, ("x", "c")).sum(axis=0)
    piece = exchanged(near, Z).sum(axis=0)
    sent = jnp.concatenate([jnp.broadcast_to(piece[None], ride.shape), ride], axis=2)
    arrived = exchanged(sent, ("x", "y"))

    cut, mapped, lifted_two, piece, other = pl.pallas_call(
        second_kernel,
        out_shape=(shape(NX * NL * NC, NH, 1, WIDE), small, small, row, row),
        in_specs=[VM, VM, hbm],
        out_specs=[VM] * 5,
        scratch_shapes=scratch,
        compiler_params=params,
        name="second_product",
    )(arrived, matrix, inputs[4])

    def call(kernel, name, out_shape, *operands):
        return pl.pallas_call(
            kernel,
            out_shape=out_shape,
            in_specs=[VM] * len(operands),
            out_specs=jax.tree.map(lambda _: VM, out_shape),
            compiler_params=light,
            name=name,
        )(*operands)

    sent = call(share_kernel, "share", shape(NH, NH + 2, 1, WIDE), exchanged(cut, ("x", "zl", "c")), piece, other)
    sent = call(dots_kernel, "dots", shape(NX * NL * NC * NY, 1, WIDE + LANE), exchanged(sent, "zh"))
    arrived = exchanged(sent, ("x", "zl", "c", "y"))
    return call(last_kernel, "update", (small, small), arrived, iterate, residual, mapped, lifted, lifted_two)


def solution(mesh):
    torus = Mesh(mesh.devices.reshape(NX, NH, NL, NC, NY), (*ROWS, "y"))
    placed = (P(ROWS, "y"), P(ROWS, None, None), P(ROWS, None), P(None, ROWS), P(None, ROWS))
    return jax.shard_map(
        body, mesh=torus, in_specs=placed, out_specs=(P(None, ROWS), P(None, ROWS)), check_vma=False
    )
```

```python
import functools

import jax
import jax.numpy as jnp
from jax import lax
from jax.experimental import pallas as pl
from jax.experimental.pallas import tpu as pltpu
from jax.sharding import Mesh
from jax.sharding import PartitionSpec as P

Z = ("zh", "zl")
ROWS = ("x", *Z, "c")
NX, NH, NL, NC, NY = 4, 8, 2, 2, 4
NZ = NH * NL
SYS, UNK, LANE = 6, 192, 128
REST = UNK - LANE
PAIR = 2
WIDE = PAIR * UNK
TILES = WIDE // LANE
BLOCKS = 24
COPIES = 4
DOTS = 6

highest = lax.Precision.HIGHEST
f32 = jnp.float32
VM = pl.BlockSpec(memory_space=pltpu.VMEM)


def iota(shape, dim):
    return lax.broadcasted_iota(jnp.int32, shape, dim)


def nt(a, b):
    return lax.dot_general(a, b, (((1,), (1,)), ((), ())), precision=highest, preferred_element_type=f32)


def preconditioner(len_ref, inverse):
    slots = BLOCKS * BLOCKS
    slot = iota((1, slots), 1)
    block = slot // BLOCKS
    within = slot - block * BLOCKS
    column = iota((1, UNK), 1)
    target = jnp.full((1, slots), -1, jnp.int32)
    first = jnp.zeros((1, UNK), jnp.int32)
    last = jnp.zeros((1, UNK), jnp.int32)
    start = jnp.int32(0)
    for b in range(BLOCKS):
        size = len_ref[0, b]
        end = start + size
        target = jnp.where((block == b) & (within < size), start + within, target)
        inside = (column >= start) & (column < end)
        first = jnp.where(inside, start, first)
        last = jnp.where(inside, end, last)
        start = end
    pick = (iota((UNK, slots), 0) == target).astype(f32)
    rows = jnp.dot(pick, inverse, precision=highest, preferred_element_type=f32)
    spread = (iota((BLOCKS, UNK), 0) == column - first).astype(f32)
    full = jnp.dot(rows, spread, precision=highest, preferred_element_type=f32)
    row = iota((UNK, UNK), 0)
    return jnp.where((row >= first) & (row < last), full, 0.0)


def encoded(vector, core):
    main = jnp.where(core == 0, vector[:, :LANE], vector[:, REST:])
    rest = jnp.where(core == 0, vector[:, LANE:], vector[:, :REST])
    rows = []
    for p in range(SYS // PAIR):
        a, b = PAIR * p, PAIR * p + 1
        rows.append(jnp.concatenate([main[a : a + 1], main[b : b + 1], rest[a : a + 1], rest[b : b + 1]], axis=1))
    return rows


def decoded(rows, core):
    main = jnp.concatenate([r[:, k * LANE : (k + 1) * LANE] for r in rows for k in range(PAIR)], axis=0)
    rest = jnp.concatenate(
        [r[:, PAIR * LANE + k * REST : PAIR * LANE + (k + 1) * REST] for r in rows for k in range(PAIR)], axis=0
    )
    return jnp.where(
        core == 0, jnp.concatenate([main, rest], axis=1), jnp.concatenate([rest, main], axis=1)
    )


def copies_of(operator_ref, held, sems):
    width = operator_ref.shape[1] // COPIES
    return [
        pltpu.make_async_copy(
            operator_ref.at[:, k * width : (k + 1) * width], held.at[:, k * width : (k + 1) * width], sems.at[k]
        )
        for k in range(COPIES)
    ]


def product(matrix, vector, copies, held, spread, cut_ref, home):
    turned = nt(matrix, vector)
    for s in range(SYS):
        spread[s] = jnp.broadcast_to(turned[:, s : s + 1], (UNK, LANE))
    low = iota((1, LANE), 1) < REST

    def one(z, carry):
        base = pl.multiple_of(z * (NC * UNK), LANE)
        totals = [[None] * TILES for _ in range(SYS)]
        for j in range(UNK // 8):
            tiles = [held[8 * j : 8 * j + 8, pl.ds(base + k * LANE, LANE)] for k in range(TILES)]
            for s in range(SYS):
                v = spread[s, 8 * j : 8 * j + 8, :]
                for k in range(TILES):
                    term = tiles[k] * v
                    totals[s][k] = term if j == 0 else totals[s][k] + term
        sums = [[jnp.sum(totals[s][k], axis=0, keepdims=True) for k in range(TILES)] for s in range(SYS)]
        for p in range(SYS // PAIR):
            a, b = sums[PAIR * p], sums[PAIR * p + 1]
            lo = jnp.where(low, a[1], pltpu.roll(b[1], REST, 1))
            hi = jnp.where(low, pltpu.roll(a[1], REST, 1), b[1])
            for c, row in ((0, (a[0], b[0], lo)), (1, (a[2], b[2], hi))):
                for k in range(TILES):
                    cut_ref[*home(p, z, c), :, k * LANE : (k + 1) * LANE] = row[k]
        return carry

    per = NZ // COPIES
    for k in range(COPIES):
        copies[k].wait()
        lax.fori_loop(k * per, (k + 1) * per, one, 0)


def first_kernel(
    len_hbm, inverse_hbm, residual_hbm, iterate_hbm, operator_hbm,
    cut_ref, matrix_ref, lifted_ref, residual_ref, iterate_ref,
    held, spread, sems, lengths, inverse, small_sems,
):
    small = [
        pltpu.make_async_copy(source, target, small_sems.at[k])
        for k, (source, target) in enumerate(
            ((len_hbm, lengths), (inverse_hbm, inverse), (residual_hbm, residual_ref), (iterate_hbm, iterate_ref))
        )
    ]
    for copy in small:
        copy.start()
    copies = copies_of(operator_hbm, held, sems)
    for copy in copies:
        copy.start()
    for copy in small:
        copy.wait()
    residual = residual_ref[...]
    matrix = preconditioner(lengths, inverse[...])
    product(matrix, residual, copies, held, spread, cut_ref, lambda p, z, c: (z, c * (SYS // PAIR) + p))
    matrix_ref[...] = matrix
    lifted_ref[...] = nt(residual, matrix)


def forward_kernel(arrived_ref, sent_ref):
    rows = jnp.sum(arrived_ref[...], axis=0)
    pairs = SYS // PAIR
    for k in range(NX * NC * NY):
        c = k // NY % NC
        sent_ref[k] = rows[c * pairs : (c + 1) * pairs]


def second_kernel(
    arrived_ref, matrix_ref, residual_ref, operator_hbm, cut_ref, mapped_ref, lifted_ref, held, spread, sems
):
    copies = copies_of(operator_hbm, held, sems)
    for copy in copies:
        copy.start()
    core, x = lax.axis_index("c"), lax.axis_index("x")
    total = None
    for k in range(NX * NC):
        part = arrived_ref[k * NY + x]
        total = part if total is None else total + part
    mapped = decoded([total[p] for p in range(SYS // PAIR)], core)
    matrix = matrix_ref[...]
    product(
        matrix, mapped, copies, held, spread, cut_ref,
        lambda p, z, c: ((p * NL + lax.rem(z, NL)) * NC + c, lax.div(z, NL)),
    )
    extra = [encoded(v, core) for v in (mapped, residual_ref[...])]
    for k in range(NX * NL * NC):
        p = k // (NL * NC)
        if p < SYS // PAIR:
            for e in range(len(extra)):
                cut_ref[k, NH + e] = extra[e][p]
        else:
            cut_ref[k] = jnp.zeros((NH + 2, 1, WIDE), f32)
    mapped_ref[...] = mapped
    lifted_ref[...] = nt(mapped, matrix)


def share_kernel(arrived_ref, sent_ref):
    near = jnp.sum(arrived_ref[:, :NH], axis=0)
    own = (lax.axis_index("y") * NL + lax.axis_index("zl")) * NC + lax.axis_index("c")
    extra = arrived_ref[own, NH:]
    for k in range(NH):
        sent_ref[k, :NH] = near
        sent_ref[k, NH:] = extra


def dots_kernel(far_ref, sent_ref):
    mine = far_ref[0, lax.axis_index("zh")]
    for k in range(1, NH):
        mine = mine + far_ref[k, lax.axis_index("zh")]
    terms = [None] * DOTS
    for h in range(NH):
        t = far_ref[0, h]
        for k in range(1, NH):
            t = t + far_ref[k, h]
        m, r = far_ref[h, NH], far_ref[h, NH + 1]
        for d, term in enumerate((r * r, r * m, m * m, t * r, t * m, t * t)):
            terms[d] = term if h == 0 else terms[d] + term
    terms = jnp.concatenate(terms, axis=0)
    shared = terms[:, PAIR * LANE :]
    low = iota(shared.shape, 1) < REST
    sides = jnp.concatenate(
        [terms[:, :LANE] + jnp.where(low, shared, 0.0), terms[:, LANE : 2 * LANE] + jnp.where(low, 0.0, shared)], axis=0
    )
    column = jnp.sum(sides, axis=1, keepdims=True)
    shape = (PAIR * DOTS, LANE)
    line = jnp.sum(jnp.where(iota(shape, 0) == iota(shape, 1), column, 0.0), axis=0, keepdims=True)
    row = jnp.concatenate([mine, line], axis=1)
    for k in range(sent_ref.shape[0]):
        sent_ref[k] = row


def last_kernel(arrived_ref, iterate_ref, residual_ref, mapped_ref, lifted_ref, lifted_two_ref, new_iterate_ref, new_residual_ref):
    core, x, low = lax.axis_index("c"), lax.axis_index("x"), lax.axis_index("zl")
    group = NL * NC * NY
    totals = None
    for k in range(NX):
        line = jnp.sum(arrived_ref[k * group : (k + 1) * group, :, WIDE:], axis=0)
        if k:
            line = pltpu.roll(line, k * PAIR * DOTS, 1)
        totals = line if totals is None else totals + line
    lane = iota((SYS, LANE), 1)
    system = iota((SYS, LANE), 0)
    home = (system // PAIR) * (PAIR * DOTS) + (system % PAIR) * DOTS
    norm_res, curve_one, square_map, mixed_res, mixed_map, square_two = (
        jnp.sum(jnp.where(lane == home + d, totals, 0.0), axis=1, keepdims=True) for d in range(DOTS)
    )
    alpha = norm_res / curve_one
    cross_mid = curve_one - alpha * square_map - alpha * mixed_res + alpha * alpha * mixed_map
    square_mid = square_map - 2.0 * alpha * mixed_map + alpha * alpha * square_two
    omega = cross_mid / square_mid
    mapped, lifted = mapped_ref[...], lifted_ref[...]
    home = (low * NC + core) * NY + x
    mapped_two = decoded([arrived_ref[p * group + home][:, :WIDE] for p in range(SYS // PAIR)], core)
    middle = residual_ref[...] - alpha * mapped
    lifted_mid = lifted - alpha * lifted_two_ref[...]
    new_iterate_ref[...] = iterate_ref[...] + alpha * lifted + omega * lifted_mid
    new_residual_ref[...] = middle - omega * (mapped - alpha * mapped_two)


def exchanged(pieces, axes):
    return lax.all_to_all(pieces, axes, split_axis=0, concat_axis=0, tiled=True)


def body(operator, block_inverse, block_len, iterate, residual):
    def shape(*lengths):
        return jax.ShapeDtypeStruct(lengths, f32)

    hbm = pl.BlockSpec(memory_space=pltpu.HBM)
    small = shape(SYS, UNK)
    scratch = [
        pltpu.VMEM(operator.shape, f32),
        pltpu.VMEM((SYS, UNK, LANE), f32),
        pltpu.SemaphoreType.DMA((COPIES,)),
    ]
    params = pltpu.CompilerParams(vmem_limit_bytes=16 << 20)
    light = pltpu.CompilerParams(vmem_limit_bytes=4 << 20)
    inputs = (block_len, block_inverse.reshape(BLOCKS * BLOCKS, BLOCKS), residual, iterate, operator)
    inputs = [pltpu.with_memory_space_constraint(a, pltpu.HBM) for a in inputs]

    cut, matrix, lifted, residual, iterate = pl.pallas_call(
        first_kernel,
        out_shape=(shape(NZ, NC * SYS // PAIR, 1, WIDE), shape(UNK, UNK), small, small, small),
        in_specs=[hbm] * 5,
        out_specs=[VM] * 5,
        scratch_shapes=scratch
        + [
            pltpu.SMEM((1, BLOCKS), jnp.int32),
            pltpu.VMEM((BLOCKS * BLOCKS, BLOCKS), f32),
            pltpu.SemaphoreType.DMA((4,)),
        ],
        compiler_params=params,
        name="first_product",
    )(*inputs)

    def call(kernel, name, out_shape, *operands):
        return pl.pallas_call(
            kernel,
            out_shape=out_shape,
            in_specs=[VM] * len(operands),
            out_specs=jax.tree.map(lambda _: VM, out_shape),
            compiler_params=light,
            name=name,
        )(*operands)

    sent = call(forward_kernel, "forward", shape(NX * NC * NY, SYS // PAIR, 1, WIDE), exchanged(cut, Z))
    arrived = exchanged(sent, ("x", "c", "y"))

    cut, mapped, lifted_two = pl.pallas_call(
        second_kernel,
        out_shape=(shape(NX * NL * NC, NH + 2, 1, WIDE), small, small),
        in_specs=[VM, VM, VM, hbm],
        out_specs=[VM] * 3,
        scratch_shapes=scratch,
        compiler_params=params,
        name="second_product",
    )(arrived, matrix, residual, inputs[4])

    sent = call(share_kernel, "share", shape(NH, NH + 2, 1, WIDE), exchanged(cut, ("x", "zl", "c")))
    sent = call(dots_kernel, "dots", shape(NX * NL * NC * NY, 1, WIDE + LANE), exchanged(sent, "zh"))
    arrived = exchanged(sent, ("x", "zl", "c", "y"))
    return call(last_kernel, "update", (small, small), arrived, iterate, residual, mapped, lifted, lifted_two)


def solution(mesh):
    torus = Mesh(mesh.devices.reshape(NX, NH, NL, NC, NY), (*ROWS, "y"))
    placed = (P(ROWS, "y"), P(ROWS, None, None), P(ROWS, None), P(None, ROWS), P(None, ROWS))
    return jax.shard_map(
        body, mesh=torus, in_specs=placed, out_specs=(P(None, ROWS), P(None, ROWS)), check_vma=False
    )
```

```python
import functools

import jax
import jax.numpy as jnp
from jax import lax
from jax.experimental import pallas as pl
from jax.experimental.pallas import tpu as pltpu
from jax.sharding import Mesh
from jax.sharding import PartitionSpec as P

Z = ("zh", "zl")
ROWS = ("x", *Z, "c")
NX, NH, NL, NC, NY = 4, 8, 2, 2, 4
NZ = NH * NL
SYS, UNK, LANE = 6, 192, 128
REST = UNK - LANE
PAIR = 2
WIDE = PAIR * UNK
TILES = WIDE // LANE
BLOCKS = 24
COPIES = 4
TOGETHER = 2
DOTS = 6

highest = lax.Precision.HIGHEST
f32, bf16 = jnp.float32, jnp.bfloat16
VM = pl.BlockSpec(memory_space=pltpu.VMEM)


def iota(shape, dim):
    return lax.broadcasted_iota(jnp.int32, shape, dim)


def nt(a, b):
    return lax.dot_general(a, b, (((1,), (1,)), ((), ())), precision=highest, preferred_element_type=f32)


def split(value):
    high = value.astype(bf16)
    left = value - high.astype(f32)
    middle = left.astype(bf16)
    return high, middle, (left - middle.astype(f32)).astype(bf16)


def one_pass(a, b):
    return jnp.dot(a, b, preferred_element_type=f32)


def preconditioner(len_ref, inverse):
    slots = BLOCKS * BLOCKS
    slot = iota((1, slots), 1)
    block = slot // BLOCKS
    within = slot - block * BLOCKS
    column = iota((1, UNK), 1)
    target = jnp.full((1, slots), -1, jnp.int32)
    first = jnp.zeros((1, UNK), jnp.int32)
    last = jnp.zeros((1, UNK), jnp.int32)
    start = jnp.int32(0)
    for b in range(BLOCKS):
        size = len_ref[0, b]
        end = start + size
        target = jnp.where((block == b) & (within < size), start + within, target)
        inside = (column >= start) & (column < end)
        first = jnp.where(inside, start, first)
        last = jnp.where(inside, end, last)
        start = end
    pick = (iota((UNK, slots), 0) == target).astype(f32).astype(bf16)
    rows = sum(one_pass(pick, part) for part in split(inverse))
    spread = (iota((BLOCKS, UNK), 0) == column - first).astype(f32).astype(bf16)
    full = sum(one_pass(part, spread) for part in split(rows))
    row = iota((UNK, UNK), 0)
    return jnp.where((row >= first) & (row < last), full, 0.0)


def encoded(vector, core):
    main = jnp.where(core == 0, vector[:, :LANE], vector[:, REST:])
    rest = jnp.where(core == 0, vector[:, LANE:], vector[:, :REST])
    rows = []
    for p in range(SYS // PAIR):
        a, b = PAIR * p, PAIR * p + 1
        rows.append(jnp.concatenate([main[a : a + 1], main[b : b + 1], rest[a : a + 1], rest[b : b + 1]], axis=1))
    return rows


def decoded(rows, core):
    main = jnp.concatenate([r[:, k * LANE : (k + 1) * LANE] for r in rows for k in range(PAIR)], axis=0)
    rest = jnp.concatenate(
        [r[:, PAIR * LANE + k * REST : PAIR * LANE + (k + 1) * REST] for r in rows for k in range(PAIR)], axis=0
    )
    return jnp.where(
        core == 0, jnp.concatenate([main, rest], axis=1), jnp.concatenate([rest, main], axis=1)
    )


def copies_of(operator_ref, held, sems):
    width = operator_ref.shape[1] // COPIES

    def copy_of(k):
        columns = pl.ds(pl.multiple_of(k * width, LANE), width)
        return pltpu.make_async_copy(operator_ref.at[:, columns], held.at[:, columns], sems.at[k])

    return copy_of


def product(matrix, vector, lifted_ref, copy_of, held, spread, cut_ref, home):
    lifted = nt(vector, matrix)
    lifted_ref[...] = lifted
    turned = lifted.T
    for s in range(SYS):
        spread[s] = jnp.broadcast_to(turned[:, s : s + 1], (UNK, LANE))
    low = iota((1, LANE), 1) < REST

    def one(step, carry):
        totals = [[[None] * TILES for _ in range(SYS)] for _ in range(TOGETHER)]
        base = pl.multiple_of(step * (TOGETHER * NC * UNK), LANE)
        for j in range(UNK // 8):
            for s in range(SYS):
                v = spread[s, 8 * j : 8 * j + 8, :]
                for g in range(TOGETHER):
                    for k in range(TILES):
                        term = held[8 * j : 8 * j + 8, pl.ds(base + (g * TILES + k) * LANE, LANE)] * v
                        totals[g][s][k] = term if j == 0 else totals[g][s][k] + term
        for g in range(TOGETHER):
            z = step * TOGETHER + g
            sums = [[jnp.sum(totals[g][s][k], axis=0, keepdims=True) for k in range(TILES)] for s in range(SYS)]
            for p in range(SYS // PAIR):
                a, b = sums[PAIR * p], sums[PAIR * p + 1]
                lo = jnp.where(low, a[1], pltpu.roll(b[1], REST, 1))
                hi = jnp.where(low, pltpu.roll(a[1], REST, 1), b[1])
                for c, row in ((0, (a[0], b[0], lo)), (1, (a[2], b[2], hi))):
                    for k in range(TILES):
                        cut_ref[*home(p, z, c), :, k * LANE : (k + 1) * LANE] = row[k]
        return carry

    per = NZ // COPIES // TOGETHER

    def chunk(k, carry):
        copy_of(k).wait()
        return lax.fori_loop(k * per, (k + 1) * per, one, carry)

    lax.fori_loop(0, COPIES, chunk, 0)


def first_kernel(
    len_hbm, inverse_hbm, residual_hbm, iterate_hbm, operator_hbm,
    cut_ref, matrix_ref, lifted_ref, residual_ref, iterate_ref,
    held, spread, sems, lengths, inverse, small_sems,
):
    small = [
        pltpu.make_async_copy(source, target, small_sems.at[k])
        for k, (source, target) in enumerate(
            ((len_hbm, lengths), (inverse_hbm, inverse), (residual_hbm, residual_ref), (iterate_hbm, iterate_ref))
        )
    ]
    for copy in small:
        copy.start()
    copy_of = copies_of(operator_hbm, held, sems)
    copy_of(0).start()
    for copy in small:
        copy.wait()
    for k in range(1, COPIES):
        copy_of(k).start()
    residual = residual_ref[...]
    matrix = preconditioner(lengths, inverse[...])
    product(matrix, residual, lifted_ref, copy_of, held, spread, cut_ref, lambda p, z, c: (z, c * (SYS // PAIR) + p))
    matrix_ref[...] = matrix


def forward_kernel(arrived_ref, sent_ref):
    rows = jnp.sum(arrived_ref[...], axis=0)
    pairs = SYS // PAIR
    for k in range(NX * NC * NY):
        c = k // NY % NC
        sent_ref[k] = rows[c * pairs : (c + 1) * pairs]


def second_kernel(
    arrived_ref, matrix_ref, residual_ref, operator_hbm, cut_ref, mapped_ref, lifted_ref, held, spread, sems
):
    copy_of = copies_of(operator_hbm, held, sems)
    for k in range(COPIES):
        copy_of(k).start()
    core, x = lax.axis_index("c"), lax.axis_index("x")
    total = None
    for k in range(NX * NC):
        part = arrived_ref[k * NY + x]
        total = part if total is None else total + part
    mapped = decoded([total[p] for p in range(SYS // PAIR)], core)
    matrix = matrix_ref[...]
    product(
        matrix, mapped, lifted_ref, copy_of, held, spread, cut_ref,
        lambda p, z, c: ((p * NL + lax.rem(z, NL)) * NC + c, lax.div(z, NL)),
    )
    extra = [encoded(v, core) for v in (mapped, residual_ref[...])]
    for k in range(NX * NL * NC):
        p = k // (NL * NC)
        if p < SYS // PAIR:
            for e in range(len(extra)):
                cut_ref[k, NH + e] = extra[e][p]
        else:
            cut_ref[k] = jnp.zeros((NH + 2, 1, WIDE), f32)
    mapped_ref[...] = mapped


def share_kernel(arrived_ref, sent_ref):
    near = jnp.sum(arrived_ref[:, :NH], axis=0)
    own = (lax.axis_index("y") * NL + lax.axis_index("zl")) * NC + lax.axis_index("c")
    extra = arrived_ref[own, NH:]
    for k in range(NH):
        sent_ref[k, :NH] = near
        sent_ref[k, NH:] = extra


def dots_kernel(far_ref, sent_ref):
    mine = far_ref[0, lax.axis_index("zh")]
    for k in range(1, NH):
        mine = mine + far_ref[k, lax.axis_index("zh")]
    terms = [None] * DOTS
    for h in range(NH):
        t = far_ref[0, h]
        for k in range(1, NH):
            t = t + far_ref[k, h]
        m, r = far_ref[h, NH], far_ref[h, NH + 1]
        for d, term in enumerate((r * r, r * m, m * m, t * r, t * m, t * t)):
            terms[d] = term if h == 0 else terms[d] + term
    terms = jnp.concatenate(terms, axis=0)
    shared = terms[:, PAIR * LANE :]
    low = iota(shared.shape, 1) < REST
    sides = jnp.concatenate(
        [terms[:, :LANE] + jnp.where(low, shared, 0.0), terms[:, LANE : 2 * LANE] + jnp.where(low, 0.0, shared)], axis=0
    )
    column = jnp.sum(sides, axis=1, keepdims=True)
    shape = (PAIR * DOTS, LANE)
    line = jnp.sum(jnp.where(iota(shape, 0) == iota(shape, 1), column, 0.0), axis=0, keepdims=True)
    row = jnp.concatenate([mine, line], axis=1)
    for k in range(sent_ref.shape[0]):
        sent_ref[k] = row


def last_kernel(arrived_ref, iterate_ref, residual_ref, mapped_ref, lifted_ref, lifted_two_ref, new_iterate_ref, new_residual_ref):
    core, x, low = lax.axis_index("c"), lax.axis_index("x"), lax.axis_index("zl")
    group = NL * NC * NY
    totals = None
    for k in range(NX):
        line = jnp.sum(arrived_ref[k * group : (k + 1) * group, :, WIDE:], axis=0)
        if k:
            line = pltpu.roll(line, k * PAIR * DOTS, 1)
        totals = line if totals is None else totals + line
    lane = iota((SYS, LANE), 1)
    system = iota((SYS, LANE), 0)
    home = (system // PAIR) * (PAIR * DOTS) + (system % PAIR) * DOTS
    norm_res, curve_one, square_map, mixed_res, mixed_map, square_two = (
        jnp.sum(jnp.where(lane == home + d, totals, 0.0), axis=1, keepdims=True) for d in range(DOTS)
    )
    alpha = norm_res / curve_one
    cross_mid = curve_one - alpha * square_map - alpha * mixed_res + alpha * alpha * mixed_map
    square_mid = square_map - 2.0 * alpha * mixed_map + alpha * alpha * square_two
    omega = cross_mid / square_mid
    mapped, lifted = mapped_ref[...], lifted_ref[...]
    home = (low * NC + core) * NY + x
    mapped_two = decoded([arrived_ref[p * group + home][:, :WIDE] for p in range(SYS // PAIR)], core)
    middle = residual_ref[...] - alpha * mapped
    lifted_mid = lifted - alpha * lifted_two_ref[...]
    new_iterate_ref[...] = iterate_ref[...] + alpha * lifted + omega * lifted_mid
    new_residual_ref[...] = middle - omega * (mapped - alpha * mapped_two)


def exchanged(pieces, axes):
    return lax.all_to_all(pieces, axes, split_axis=0, concat_axis=0, tiled=True)


def body(operator, block_inverse, block_len, iterate, residual):
    def shape(*lengths):
        return jax.ShapeDtypeStruct(lengths, f32)

    hbm = pl.BlockSpec(memory_space=pltpu.HBM)
    small = shape(SYS, UNK)
    scratch = [
        pltpu.VMEM(operator.shape, f32),
        pltpu.VMEM((SYS, UNK, LANE), f32),
        pltpu.SemaphoreType.DMA((COPIES,)),
    ]
    params = pltpu.CompilerParams(vmem_limit_bytes=16 << 20)
    light = pltpu.CompilerParams(vmem_limit_bytes=4 << 20)
    inputs = (block_len, block_inverse.reshape(BLOCKS * BLOCKS, BLOCKS), residual, iterate, operator)
    inputs = [pltpu.with_memory_space_constraint(a, pltpu.HBM) for a in inputs]

    cut, matrix, lifted, residual, iterate = pl.pallas_call(
        first_kernel,
        out_shape=(shape(NZ, NC * SYS // PAIR, 1, WIDE), shape(UNK, UNK), small, small, small),
        in_specs=[hbm] * 5,
        out_specs=[VM] * 5,
        scratch_shapes=scratch
        + [
            pltpu.SMEM((1, BLOCKS), jnp.int32),
            pltpu.VMEM((BLOCKS * BLOCKS, BLOCKS), f32),
            pltpu.SemaphoreType.DMA((4,)),
        ],
        compiler_params=params,
        name="first_product",
    )(*inputs)

    def call(kernel, name, out_shape, *operands):
        return pl.pallas_call(
            kernel,
            out_shape=out_shape,
            in_specs=[VM] * len(operands),
            out_specs=jax.tree.map(lambda _: VM, out_shape),
            compiler_params=light,
            name=name,
        )(*operands)

    sent = call(forward_kernel, "forward", shape(NX * NC * NY, SYS // PAIR, 1, WIDE), exchanged(cut, Z))
    arrived = exchanged(sent, ("x", "c", "y"))

    cut, mapped, lifted_two = pl.pallas_call(
        second_kernel,
        out_shape=(shape(NX * NL * NC, NH + 2, 1, WIDE), small, small),
        in_specs=[VM, VM, VM, hbm],
        out_specs=[VM] * 3,
        scratch_shapes=scratch,
        compiler_params=params,
        name="second_product",
    )(arrived, matrix, residual, inputs[4])

    sent = call(share_kernel, "share", shape(NH, NH + 2, 1, WIDE), exchanged(cut, ("x", "zl", "c")))
    sent = call(dots_kernel, "dots", shape(NX * NL * NC * NY, 1, WIDE + LANE), exchanged(sent, "zh"))
    arrived = exchanged(sent, ("x", "zl", "c", "y"))
    return call(last_kernel, "update", (small, small), arrived, iterate, residual, mapped, lifted, lifted_two)


def solution(mesh):
    torus = Mesh(mesh.devices.reshape(NX, NH, NL, NC, NY), (*ROWS, "y"))
    placed = (P(ROWS, "y"), P(ROWS, None, None), P(ROWS, None), P(None, ROWS), P(None, ROWS))
    return jax.shard_map(
        body, mesh=torus, in_specs=placed, out_specs=(P(None, ROWS), P(None, ROWS)), check_vma=False
    )
```

```python
import functools

import jax
import jax.numpy as jnp
from jax import lax
from jax.experimental import pallas as pl
from jax.experimental.pallas import tpu as pltpu
from jax.sharding import Mesh
from jax.sharding import PartitionSpec as P

Z = ("zh", "zl")
ROWS = ("x", *Z, "c")
NX, NH, NL, NC, NY = 4, 8, 2, 2, 4
NZ = NH * NL
SYS, UNK, LANE = 6, 192, 128
REST = UNK - LANE
PAIR = 2
WIDE = PAIR * UNK
TILES = WIDE // LANE
BLOCKS = 24
COPIES = 4
TOGETHER = 2
DOTS = 6
PAIRS = SYS // PAIR
EACH = PAIRS * NH // NX

highest = lax.Precision.HIGHEST
f32, bf16 = jnp.float32, jnp.bfloat16
VM = pl.BlockSpec(memory_space=pltpu.VMEM)


def iota(shape, dim):
    return lax.broadcasted_iota(jnp.int32, shape, dim)


def nt(a, b):
    return lax.dot_general(a, b, (((1,), (1,)), ((), ())), precision=highest, preferred_element_type=f32)


def split(value):
    high = value.astype(bf16)
    left = value - high.astype(f32)
    middle = left.astype(bf16)
    return high, middle, (left - middle.astype(f32)).astype(bf16)


def one_pass(a, b):
    return jnp.dot(a, b, preferred_element_type=f32)


def preconditioner(len_ref, inverse):
    slots = BLOCKS * BLOCKS
    slot = iota((1, slots), 1)
    block = slot // BLOCKS
    within = slot - block * BLOCKS
    column = iota((1, UNK), 1)
    target = jnp.full((1, slots), -1, jnp.int32)
    first = jnp.zeros((1, UNK), jnp.int32)
    last = jnp.zeros((1, UNK), jnp.int32)
    start = jnp.int32(0)
    for b in range(BLOCKS):
        size = len_ref[0, b]
        end = start + size
        target = jnp.where((block == b) & (within < size), start + within, target)
        inside = (column >= start) & (column < end)
        first = jnp.where(inside, start, first)
        last = jnp.where(inside, end, last)
        start = end
    pick = (iota((UNK, slots), 0) == target).astype(f32).astype(bf16)
    rows = sum(one_pass(pick, part) for part in split(inverse))
    spread = (iota((BLOCKS, UNK), 0) == column - first).astype(f32).astype(bf16)
    full = sum(one_pass(part, spread) for part in split(rows))
    row = iota((UNK, UNK), 0)
    return jnp.where((row >= first) & (row < last), full, 0.0)


def encoded(vector, core):
    main = jnp.where(core == 0, vector[:, :LANE], vector[:, REST:])
    rest = jnp.where(core == 0, vector[:, LANE:], vector[:, :REST])
    rows = []
    for p in range(PAIRS):
        a, b = PAIR * p, PAIR * p + 1
        rows.append(jnp.concatenate([main[a : a + 1], main[b : b + 1], rest[a : a + 1], rest[b : b + 1]], axis=1))
    return rows


def decoded(rows, core):
    main = jnp.concatenate([r[:, k * LANE : (k + 1) * LANE] for r in rows for k in range(PAIR)], axis=0)
    rest = jnp.concatenate(
        [r[:, PAIR * LANE + k * REST : PAIR * LANE + (k + 1) * REST] for r in rows for k in range(PAIR)], axis=0
    )
    return jnp.where(
        core == 0, jnp.concatenate([main, rest], axis=1), jnp.concatenate([rest, main], axis=1)
    )


def copies_of(operator_ref, held, sems):
    width = operator_ref.shape[1] // COPIES

    def copy_of(k):
        columns = pl.ds(pl.multiple_of(k * width, LANE), width)
        return pltpu.make_async_copy(operator_ref.at[:, columns], held.at[:, columns], sems.at[k])

    return copy_of


def product(matrix, vector, lifted_ref, copy_of, held, spread, cut_ref, home):
    lifted = nt(vector, matrix)
    lifted_ref[...] = lifted
    turned = lifted.T
    for s in range(SYS):
        spread[s] = jnp.broadcast_to(turned[:, s : s + 1], (UNK, LANE))
    low = iota((1, LANE), 1) < REST

    def one(step, carry):
        totals = [[[None] * TILES for _ in range(SYS)] for _ in range(TOGETHER)]
        base = pl.multiple_of(step * (TOGETHER * NC * UNK), LANE)
        for j in range(UNK // 8):
            for s in range(SYS):
                v = spread[s, 8 * j : 8 * j + 8, :]
                for g in range(TOGETHER):
                    for k in range(TILES):
                        term = held[8 * j : 8 * j + 8, pl.ds(base + (g * TILES + k) * LANE, LANE)] * v
                        totals[g][s][k] = term if j == 0 else totals[g][s][k] + term
        for g in range(TOGETHER):
            z = step * TOGETHER + g
            sums = [[jnp.sum(totals[g][s][k], axis=0, keepdims=True) for k in range(TILES)] for s in range(SYS)]
            for p in range(PAIRS):
                a, b = sums[PAIR * p], sums[PAIR * p + 1]
                lo = jnp.where(low, a[1], pltpu.roll(b[1], REST, 1))
                hi = jnp.where(low, pltpu.roll(a[1], REST, 1), b[1])
                for c, row in ((0, (a[0], b[0], lo)), (1, (a[2], b[2], hi))):
                    for k in range(TILES):
                        cut_ref[*home(p, z, c), :, k * LANE : (k + 1) * LANE] = row[k]
        return carry

    per = NZ // COPIES // TOGETHER

    def chunk(k, carry):
        copy_of(k).wait()
        return lax.fori_loop(k * per, (k + 1) * per, one, carry)

    lax.fori_loop(0, COPIES, chunk, 0)


def first_kernel(
    len_hbm, inverse_hbm, residual_hbm, iterate_hbm, operator_hbm,
    cut_ref, matrix_ref, lifted_ref, residual_ref, iterate_ref,
    held, spread, sems, lengths, inverse, small_sems,
):
    small = [
        pltpu.make_async_copy(source, target, small_sems.at[k])
        for k, (source, target) in enumerate(
            ((len_hbm, lengths), (inverse_hbm, inverse), (residual_hbm, residual_ref), (iterate_hbm, iterate_ref))
        )
    ]
    for copy in small:
        copy.start()
    copy_of = copies_of(operator_hbm, held, sems)
    copy_of(0).start()
    for copy in small:
        copy.wait()
    for k in range(1, COPIES):
        copy_of(k).start()
    residual = residual_ref[...]
    matrix = preconditioner(lengths, inverse[...])
    product(matrix, residual, lifted_ref, copy_of, held, spread, cut_ref, lambda p, z, c: (z, c * (PAIRS) + p))
    matrix_ref[...] = matrix


def forward_kernel(arrived_ref, sent_ref):
    rows = jnp.sum(arrived_ref[...], axis=0)
    pairs = PAIRS
    for k in range(NX * NC * NY):
        c = k // NY % NC
        sent_ref[k] = rows[c * pairs : (c + 1) * pairs]


def second_kernel(
    arrived_ref, matrix_ref, residual_ref, operator_hbm, cut_ref, mapped_ref, lifted_ref, held, spread, sems
):
    copy_of = copies_of(operator_hbm, held, sems)
    for k in range(COPIES):
        copy_of(k).start()
    core, x = lax.axis_index("c"), lax.axis_index("x")
    total = None
    for k in range(NX * NC):
        part = arrived_ref[k * NY + x]
        total = part if total is None else total + part
    mapped = decoded([total[p] for p in range(PAIRS)], core)
    matrix = matrix_ref[...]

    def home(p, z, c):
        row = p * NH + lax.div(z, NL)
        x = lax.div(row, EACH)
        return (x * NL + lax.rem(z, NL)) * NC + c, row - x * EACH

    product(matrix, mapped, lifted_ref, copy_of, held, spread, cut_ref, home)
    step = lax.axis_index("zh")
    for e, vector in enumerate((mapped, residual_ref[...])):
        extra = encoded(vector, core)
        for to in range(NX):
            row = jnp.zeros((1, WIDE), f32)
            for p in range(PAIRS):
                at = p * NH + step - to * EACH
                row = jnp.where((at >= 0) & (at < EACH), extra[p], row)
            for k in range(NL * NC):
                cut_ref[to * NL * NC + k, EACH + e] = row
    mapped_ref[...] = mapped


def share_kernel(arrived_ref, sent_ref):
    near = jnp.sum(arrived_ref[:, :EACH], axis=0)
    own = (lax.axis_index("y") * NL + lax.axis_index("zl")) * NC + lax.axis_index("c")
    extra = arrived_ref[own, EACH:]
    for k in range(NH):
        sent_ref[k, :EACH] = near
        sent_ref[k, EACH:] = extra


def dots_kernel(far_ref, sent_ref):
    base = lax.axis_index("x") * EACH
    first = lax.div(base, NH)
    step = lax.axis_index("zh")
    mine = jnp.zeros((1, WIDE), f32)
    terms = [jnp.zeros((1, WIDE), f32)] * (2 * DOTS)
    for j in range(EACH):
        t = far_ref[0, j]
        for k in range(1, NH):
            t = t + far_ref[k, j]
        h = lax.rem(base + j, NH)
        mine = jnp.where(h == step, t, mine)
        m, r = far_ref[h, EACH], far_ref[h, EACH + 1]
        same = lax.div(base + j, NH) == first
        for d, term in enumerate((r * r, r * m, m * m, t * r, t * m, t * t)):
            terms[d] = terms[d] + jnp.where(same, term, 0.0)
            terms[DOTS + d] = terms[DOTS + d] + jnp.where(same, 0.0, term)
    terms = jnp.concatenate(terms, axis=0)
    main, other, shared = (terms[:, k * LANE : (k + 1) * LANE] for k in range(TILES))
    low = iota(shared.shape, 1) < REST
    main = main + jnp.where(low, shared, 0.0)
    other = other + jnp.where(low, 0.0, shared)
    column = jnp.sum(
        jnp.concatenate([main[:DOTS], other[:DOTS], main[DOTS:], other[DOTS:]], axis=0), axis=1, keepdims=True
    )
    shape = (2 * PAIR * DOTS, LANE)
    place = iota(shape, 0) + first * (PAIR * DOTS)
    line = jnp.sum(jnp.where(place == iota(shape, 1), column, 0.0), axis=0, keepdims=True)
    row = jnp.concatenate([mine, line], axis=1)
    for k in range(sent_ref.shape[0]):
        sent_ref[k] = row


def last_kernel(arrived_ref, iterate_ref, residual_ref, mapped_ref, lifted_ref, lifted_two_ref, new_iterate_ref, new_residual_ref):
    core, x = lax.axis_index("c"), lax.axis_index("x")
    totals = jnp.sum(arrived_ref[:, :, WIDE:], axis=0)
    lane = iota((SYS, LANE), 1)
    system = iota((SYS, LANE), 0)
    home = (system // PAIR) * (PAIR * DOTS) + (system % PAIR) * DOTS
    norm_res, curve_one, square_map, mixed_res, mixed_map, square_two = (
        jnp.sum(jnp.where(lane == home + d, totals, 0.0), axis=1, keepdims=True) for d in range(DOTS)
    )
    alpha = norm_res / curve_one
    cross_mid = curve_one - alpha * square_map - alpha * mixed_res + alpha * alpha * mixed_map
    square_mid = square_map - 2.0 * alpha * mixed_map + alpha * alpha * square_two
    omega = cross_mid / square_mid
    mapped, lifted = mapped_ref[...], lifted_ref[...]
    rows = []
    for p in range(PAIRS):
        source = lax.div(p * NH + lax.axis_index("zh"), EACH)
        rows.append(arrived_ref[((source * NL + lax.axis_index("zl")) * NC + core) * NY + x][:, :WIDE])
    mapped_two = decoded(rows, core)
    middle = residual_ref[...] - alpha * mapped
    lifted_mid = lifted - alpha * lifted_two_ref[...]
    new_iterate_ref[...] = iterate_ref[...] + alpha * lifted + omega * lifted_mid
    new_residual_ref[...] = middle - omega * (mapped - alpha * mapped_two)


def exchanged(pieces, axes):
    return lax.all_to_all(pieces, axes, split_axis=0, concat_axis=0, tiled=True)


def body(operator, block_inverse, block_len, iterate, residual):
    def shape(*lengths):
        return jax.ShapeDtypeStruct(lengths, f32)

    hbm = pl.BlockSpec(memory_space=pltpu.HBM)
    small = shape(SYS, UNK)
    scratch = [
        pltpu.VMEM(operator.shape, f32),
        pltpu.VMEM((SYS, UNK, LANE), f32),
        pltpu.SemaphoreType.DMA((COPIES,)),
    ]
    params = pltpu.CompilerParams(vmem_limit_bytes=16 << 20)
    light = pltpu.CompilerParams(vmem_limit_bytes=4 << 20)
    inputs = (block_len, block_inverse.reshape(BLOCKS * BLOCKS, BLOCKS), residual, iterate, operator)
    inputs = [pltpu.with_memory_space_constraint(a, pltpu.HBM) for a in inputs]

    cut, matrix, lifted, residual, iterate = pl.pallas_call(
        first_kernel,
        out_shape=(shape(NZ, NC * PAIRS, 1, WIDE), shape(UNK, UNK), small, small, small),
        in_specs=[hbm] * 5,
        out_specs=[VM] * 5,
        scratch_shapes=scratch
        + [
            pltpu.SMEM((1, BLOCKS), jnp.int32),
            pltpu.VMEM((BLOCKS * BLOCKS, BLOCKS), f32),
            pltpu.SemaphoreType.DMA((4,)),
        ],
        compiler_params=params,
        name="first_product",
    )(*inputs)

    def call(kernel, name, out_shape, *operands):
        return pl.pallas_call(
            kernel,
            out_shape=out_shape,
            in_specs=[VM] * len(operands),
            out_specs=jax.tree.map(lambda _: VM, out_shape),
            compiler_params=light,
            name=name,
        )(*operands)

    sent = call(forward_kernel, "forward", shape(NX * NC * NY, PAIRS, 1, WIDE), exchanged(cut, Z))
    arrived = exchanged(sent, ("x", "c", "y"))

    cut, mapped, lifted_two = pl.pallas_call(
        second_kernel,
        out_shape=(shape(NX * NL * NC, EACH + 2, 1, WIDE), small, small),
        in_specs=[VM, VM, VM, hbm],
        out_specs=[VM] * 3,
        scratch_shapes=scratch,
        compiler_params=params,
        name="second_product",
    )(arrived, matrix, residual, inputs[4])

    sent = call(share_kernel, "share", shape(NH, EACH + 2, 1, WIDE), exchanged(cut, ("x", "zl", "c")))
    sent = call(dots_kernel, "dots", shape(NX * NL * NC * NY, 1, WIDE + LANE), exchanged(sent, "zh"))
    arrived = exchanged(sent, ("x", "zl", "c", "y"))
    return call(last_kernel, "update", (small, small), arrived, iterate, residual, mapped, lifted, lifted_two)


def solution(mesh):
    torus = Mesh(mesh.devices.reshape(NX, NH, NL, NC, NY), (*ROWS, "y"))
    placed = (P(ROWS, "y"), P(ROWS, None, None), P(ROWS, None), P(None, ROWS), P(None, ROWS))
    return jax.shard_map(
        body, mesh=torus, in_specs=placed, out_specs=(P(None, ROWS), P(None, ROWS)), check_vma=False
    )
```

```python
import functools

import jax
import jax.numpy as jnp
from jax import lax
from jax.experimental import pallas as pl
from jax.experimental.pallas import tpu as pltpu
from jax.sharding import Mesh
from jax.sharding import PartitionSpec as P

Z = ("zh", "zl")
ROWS = ("x", *Z, "c")
NX, NH, NL, NC, NY = 4, 8, 2, 2, 4
NZ = NH * NL
SYS, UNK, LANE = 6, 192, 128
REST = UNK - LANE
PAIR = 2
WIDE = PAIR * UNK
TILES = WIDE // LANE
BLOCKS = 24
COPIES = 4
TOGETHER = 2
DOTS = 6
PAIRS = SYS // PAIR
EACH = PAIRS * NH // NX

highest = lax.Precision.HIGHEST
f32, bf16 = jnp.float32, jnp.bfloat16
VM = pl.BlockSpec(memory_space=pltpu.VMEM)


def iota(shape, dim):
    return lax.broadcasted_iota(jnp.int32, shape, dim)


def nt(a, b):
    return lax.dot_general(a, b, (((1,), (1,)), ((), ())), precision=highest, preferred_element_type=f32)


def split(value):
    high = value.astype(bf16)
    left = value - high.astype(f32)
    middle = left.astype(bf16)
    return high, middle, (left - middle.astype(f32)).astype(bf16)


def one_pass(a, b):
    return jnp.dot(a, b, preferred_element_type=f32)


def preconditioner(len_ref, inverse):
    slots = BLOCKS * BLOCKS
    slot = iota((1, slots), 1)
    block = slot // BLOCKS
    within = slot - block * BLOCKS
    column = iota((1, UNK), 1)
    target = jnp.full((1, slots), -1, jnp.int32)
    first = jnp.zeros((1, UNK), jnp.int32)
    last = jnp.zeros((1, UNK), jnp.int32)
    start = jnp.int32(0)
    for b in range(BLOCKS):
        size = len_ref[0, b]
        end = start + size
        target = jnp.where((block == b) & (within < size), start + within, target)
        inside = (column >= start) & (column < end)
        first = jnp.where(inside, start, first)
        last = jnp.where(inside, end, last)
        start = end
    pick = (iota((UNK, slots), 0) == target).astype(f32).astype(bf16)
    rows = sum(one_pass(pick, part) for part in split(inverse))
    spread = (iota((BLOCKS, UNK), 0) == column - first).astype(f32).astype(bf16)
    full = sum(one_pass(part, spread) for part in split(rows))
    row = iota((UNK, UNK), 0)
    return jnp.where((row >= first) & (row < last), full, 0.0)


def encoded(vector, core):
    main = jnp.where(core == 0, vector[:, :LANE], vector[:, REST:])
    rest = jnp.where(core == 0, vector[:, LANE:], vector[:, :REST])
    rows = []
    for p in range(PAIRS):
        a, b = PAIR * p, PAIR * p + 1
        rows.append(jnp.concatenate([main[a : a + 1], main[b : b + 1], rest[a : a + 1], rest[b : b + 1]], axis=1))
    return rows


def decoded(rows, core):
    main = jnp.concatenate([r[:, k * LANE : (k + 1) * LANE] for r in rows for k in range(PAIR)], axis=0)
    rest = jnp.concatenate(
        [r[:, PAIR * LANE + k * REST : PAIR * LANE + (k + 1) * REST] for r in rows for k in range(PAIR)], axis=0
    )
    return jnp.where(
        core == 0, jnp.concatenate([main, rest], axis=1), jnp.concatenate([rest, main], axis=1)
    )


def copies_of(operator_ref, held, sems):
    width = operator_ref.shape[1] // COPIES

    def copy_of(k):
        columns = pl.ds(pl.multiple_of(k * width, LANE), width)
        return pltpu.make_async_copy(operator_ref.at[:, columns], held.at[:, columns], sems.at[k])

    return copy_of


def product(matrix, vector, lifted_ref, copy_of, held, spread, cut_ref, home):
    lifted = nt(vector, matrix)
    lifted_ref[...] = lifted
    turned = lifted.T
    for s in range(SYS):
        spread[s] = jnp.broadcast_to(turned[:, s : s + 1], (UNK, LANE))
    low = iota((1, LANE), 1) < REST

    def one(step, carry):
        totals = [[[None] * TILES for _ in range(SYS)] for _ in range(TOGETHER)]
        base = pl.multiple_of(step * (TOGETHER * NC * UNK), LANE)
        for j in range(UNK // 8):
            for s in range(SYS):
                v = spread[s, 8 * j : 8 * j + 8, :]
                for g in range(TOGETHER):
                    for k in range(TILES):
                        term = held[8 * j : 8 * j + 8, pl.ds(base + (g * TILES + k) * LANE, LANE)] * v
                        totals[g][s][k] = term if j == 0 else totals[g][s][k] + term
        for g in range(TOGETHER):
            z = step * TOGETHER + g
            sums = [[jnp.sum(totals[g][s][k], axis=0, keepdims=True) for k in range(TILES)] for s in range(SYS)]
            for p in range(PAIRS):
                a, b = sums[PAIR * p], sums[PAIR * p + 1]
                lo = jnp.where(low, a[1], pltpu.roll(b[1], REST, 1))
                hi = jnp.where(low, pltpu.roll(a[1], REST, 1), b[1])
                for c, row in ((0, (a[0], b[0], lo)), (1, (a[2], b[2], hi))):
                    for k in range(TILES):
                        cut_ref[*home(p, z, c), :, k * LANE : (k + 1) * LANE] = row[k]
        return carry

    if copy_of is None:
        lax.fori_loop(0, NZ // TOGETHER, one, 0)
        return
    per = NZ // COPIES // TOGETHER

    def chunk(k, carry):
        copy_of(k).wait()
        return lax.fori_loop(k * per, (k + 1) * per, one, carry)

    lax.fori_loop(0, COPIES, chunk, 0)


def first_kernel(
    len_hbm, inverse_hbm, residual_hbm, iterate_hbm, operator_hbm,
    cut_ref, matrix_ref, lifted_ref, residual_ref, iterate_ref, held,
    spread, sems, lengths, inverse, small_sems,
):
    small = [
        pltpu.make_async_copy(source, target, small_sems.at[k])
        for k, (source, target) in enumerate(
            ((len_hbm, lengths), (inverse_hbm, inverse), (residual_hbm, residual_ref), (iterate_hbm, iterate_ref))
        )
    ]
    for copy in small:
        copy.start()
    copy_of = copies_of(operator_hbm, held, sems)
    copy_of(0).start()
    for copy in small:
        copy.wait()
    for k in range(1, COPIES):
        copy_of(k).start()
    residual = residual_ref[...]
    matrix = preconditioner(lengths, inverse[...])
    product(matrix, residual, lifted_ref, copy_of, held, spread, cut_ref, lambda p, z, c: (z, c * (PAIRS) + p))
    matrix_ref[...] = matrix


def forward_kernel(arrived_ref, sent_ref):
    rows = jnp.sum(arrived_ref[...], axis=0)
    pairs = PAIRS
    for k in range(NX * NC * NY):
        c = k // NY % NC
        sent_ref[k] = rows[c * pairs : (c + 1) * pairs]


def second_kernel(
    arrived_ref, matrix_ref, residual_ref, held, cut_ref, mapped_ref, lifted_ref, spread
):
    core, x = lax.axis_index("c"), lax.axis_index("x")
    total = None
    for k in range(NX * NC):
        part = arrived_ref[k * NY + x]
        total = part if total is None else total + part
    mapped = decoded([total[p] for p in range(PAIRS)], core)
    matrix = matrix_ref[...]

    def home(p, z, c):
        row = p * NH + lax.div(z, NL)
        x = lax.div(row, EACH)
        return (x * NL + lax.rem(z, NL)) * NC + c, row - x * EACH

    product(matrix, mapped, lifted_ref, None, held, spread, cut_ref, home)
    step = lax.axis_index("zh")
    for e, vector in enumerate((mapped, residual_ref[...])):
        extra = encoded(vector, core)
        for to in range(NX):
            row = jnp.zeros((1, WIDE), f32)
            for p in range(PAIRS):
                at = p * NH + step - to * EACH
                row = jnp.where((at >= 0) & (at < EACH), extra[p], row)
            for k in range(NL * NC):
                cut_ref[to * NL * NC + k, EACH + e] = row
    mapped_ref[...] = mapped


def share_kernel(arrived_ref, sent_ref):
    near = jnp.sum(arrived_ref[:, :EACH], axis=0)
    own = (lax.axis_index("y") * NL + lax.axis_index("zl")) * NC + lax.axis_index("c")
    extra = arrived_ref[own, EACH:]
    for k in range(NH):
        sent_ref[k, :EACH] = near
        sent_ref[k, EACH:] = extra


def dots_kernel(far_ref, sent_ref):
    base = lax.axis_index("x") * EACH
    first = lax.div(base, NH)
    step = lax.axis_index("zh")
    mine = jnp.zeros((1, WIDE), f32)
    terms = [jnp.zeros((1, WIDE), f32)] * (2 * DOTS)
    for j in range(EACH):
        t = far_ref[0, j]
        for k in range(1, NH):
            t = t + far_ref[k, j]
        h = lax.rem(base + j, NH)
        mine = jnp.where(h == step, t, mine)
        m, r = far_ref[h, EACH], far_ref[h, EACH + 1]
        same = lax.div(base + j, NH) == first
        for d, term in enumerate((r * r, r * m, m * m, t * r, t * m, t * t)):
            terms[d] = terms[d] + jnp.where(same, term, 0.0)
            terms[DOTS + d] = terms[DOTS + d] + jnp.where(same, 0.0, term)
    terms = jnp.concatenate(terms, axis=0)
    main, other, shared = (terms[:, k * LANE : (k + 1) * LANE] for k in range(TILES))
    low = iota(shared.shape, 1) < REST
    main = main + jnp.where(low, shared, 0.0)
    other = other + jnp.where(low, 0.0, shared)
    column = jnp.sum(
        jnp.concatenate([main[:DOTS], other[:DOTS], main[DOTS:], other[DOTS:]], axis=0), axis=1, keepdims=True
    )
    shape = (2 * PAIR * DOTS, LANE)
    place = iota(shape, 0) + first * (PAIR * DOTS)
    line = jnp.sum(jnp.where(place == iota(shape, 1), column, 0.0), axis=0, keepdims=True)
    row = jnp.concatenate([mine, line], axis=1)
    for k in range(sent_ref.shape[0]):
        sent_ref[k] = row


def last_kernel(arrived_ref, iterate_ref, residual_ref, mapped_ref, lifted_ref, lifted_two_ref, new_iterate_ref, new_residual_ref):
    core, x = lax.axis_index("c"), lax.axis_index("x")
    totals = jnp.sum(arrived_ref[:, :, WIDE:], axis=0)
    lane = iota((SYS, LANE), 1)
    system = iota((SYS, LANE), 0)
    home = (system // PAIR) * (PAIR * DOTS) + (system % PAIR) * DOTS
    norm_res, curve_one, square_map, mixed_res, mixed_map, square_two = (
        jnp.sum(jnp.where(lane == home + d, totals, 0.0), axis=1, keepdims=True) for d in range(DOTS)
    )
    alpha = norm_res / curve_one
    cross_mid = curve_one - alpha * square_map - alpha * mixed_res + alpha * alpha * mixed_map
    square_mid = square_map - 2.0 * alpha * mixed_map + alpha * alpha * square_two
    omega = cross_mid / square_mid
    mapped, lifted = mapped_ref[...], lifted_ref[...]
    rows = []
    for p in range(PAIRS):
        source = lax.div(p * NH + lax.axis_index("zh"), EACH)
        rows.append(arrived_ref[((source * NL + lax.axis_index("zl")) * NC + core) * NY + x][:, :WIDE])
    mapped_two = decoded(rows, core)
    middle = residual_ref[...] - alpha * mapped
    lifted_mid = lifted - alpha * lifted_two_ref[...]
    new_iterate_ref[...] = iterate_ref[...] + alpha * lifted + omega * lifted_mid
    new_residual_ref[...] = middle - omega * (mapped - alpha * mapped_two)


def exchanged(pieces, axes):
    return lax.all_to_all(pieces, axes, split_axis=0, concat_axis=0, tiled=True)


def body(operator, block_inverse, block_len, iterate, residual):
    def shape(*lengths):
        return jax.ShapeDtypeStruct(lengths, f32)

    hbm = pl.BlockSpec(memory_space=pltpu.HBM)
    small = shape(SYS, UNK)
    scratch = [pltpu.VMEM((SYS, UNK, LANE), f32)]
    params = pltpu.CompilerParams(vmem_limit_bytes=16 << 20)
    light = pltpu.CompilerParams(vmem_limit_bytes=4 << 20)
    inputs = (block_len, block_inverse.reshape(BLOCKS * BLOCKS, BLOCKS), residual, iterate, operator)
    inputs = [pltpu.with_memory_space_constraint(a, pltpu.HBM) for a in inputs]

    cut, matrix, lifted, residual, iterate, held = pl.pallas_call(
        first_kernel,
        out_shape=(shape(NZ, NC * PAIRS, 1, WIDE), shape(UNK, UNK), small, small, small, shape(*operator.shape)),
        in_specs=[hbm] * 5,
        out_specs=[VM] * 6,
        scratch_shapes=[
            *scratch,
            pltpu.SemaphoreType.DMA((COPIES,)),
            pltpu.SMEM((1, BLOCKS), jnp.int32),
            pltpu.VMEM((BLOCKS * BLOCKS, BLOCKS), f32),
            pltpu.SemaphoreType.DMA((4,)),
        ],
        compiler_params=params,
        name="first_product",
    )(*inputs)

    def call(kernel, name, out_shape, *operands):
        return pl.pallas_call(
            kernel,
            out_shape=out_shape,
            in_specs=[VM] * len(operands),
            out_specs=jax.tree.map(lambda _: VM, out_shape),
            compiler_params=light,
            name=name,
        )(*operands)

    sent = call(forward_kernel, "forward", shape(NX * NC * NY, PAIRS, 1, WIDE), exchanged(cut, Z))
    arrived = exchanged(sent, ("x", "c", "y"))

    cut, mapped, lifted_two = pl.pallas_call(
        second_kernel,
        out_shape=(shape(NX * NL * NC, EACH + 2, 1, WIDE), small, small),
        in_specs=[VM] * 4,
        out_specs=[VM] * 3,
        scratch_shapes=scratch,
        compiler_params=params,
        name="second_product",
    )(arrived, matrix, residual, held)

    sent = call(share_kernel, "share", shape(NH, EACH + 2, 1, WIDE), exchanged(cut, ("x", "zl", "c")))
    sent = call(dots_kernel, "dots", shape(NX * NL * NC * NY, 1, WIDE + LANE), exchanged(sent, "zh"))
    arrived = exchanged(sent, ("x", "zl", "c", "y"))
    return call(last_kernel, "update", (small, small), arrived, iterate, residual, mapped, lifted, lifted_two)


def solution(mesh):
    torus = Mesh(mesh.devices.reshape(NX, NH, NL, NC, NY), (*ROWS, "y"))
    placed = (P(ROWS, "y"), P(ROWS, None, None), P(ROWS, None), P(None, ROWS), P(None, ROWS))
    return jax.shard_map(
        body, mesh=torus, in_specs=placed, out_specs=(P(None, ROWS), P(None, ROWS)), check_vma=False
    )
```

```python
import functools

import jax
import jax.numpy as jnp
from jax import lax
from jax.experimental import pallas as pl
from jax.experimental.pallas import tpu as pltpu
from jax.sharding import Mesh
from jax.sharding import PartitionSpec as P

Z = ("zh", "zl")
ROWS = ("x", *Z, "c")
NX, NH, NL, NC, NY = 4, 8, 2, 2, 4
NZ = NH * NL
SYS, UNK, LANE = 6, 192, 128
REST = UNK - LANE
PAIR = 2
WIDE = PAIR * UNK
TILES = WIDE // LANE
BLOCKS = 24
COPIES = 4
TOGETHER = 2
DOTS = 6
PAIRS = SYS // PAIR
EACH = PAIRS * NH // NX

highest = lax.Precision.HIGHEST
f32, bf16 = jnp.float32, jnp.bfloat16
VM = pl.BlockSpec(memory_space=pltpu.VMEM)


def iota(shape, dim):
    return lax.broadcasted_iota(jnp.int32, shape, dim)


def split(value):
    high = value.astype(bf16)
    left = value - high.astype(f32)
    middle = left.astype(bf16)
    return high, middle, (left - middle.astype(f32)).astype(bf16)


def one_pass(a, b):
    return jnp.dot(a, b, preferred_element_type=f32)


def nt(vector, matrix):
    padded = jnp.concatenate([vector, jnp.zeros((8 - SYS, UNK), f32)], axis=0)
    rows = jnp.concatenate([p.astype(f32) for p in split(padded)], axis=0).astype(bf16)
    total = None
    for k, part in reversed(list(enumerate(split(matrix)))):
        out = lax.dot_general(
            rows[: 8 * (TILES - k)], part, (((1,), (1,)), ((), ())), preferred_element_type=f32
        )
        for e in reversed(range(TILES - k)):
            piece = out[8 * e : 8 * e + 8]
            total = piece if total is None else total + piece
    return total[:SYS]


def preconditioner(len_ref, inverse):
    slots = BLOCKS * BLOCKS
    slot = iota((1, slots), 1)
    block = slot // BLOCKS
    within = slot - block * BLOCKS
    column = iota((1, UNK), 1)
    target = jnp.full((1, slots), -1, jnp.int32)
    first = jnp.zeros((1, UNK), jnp.int32)
    last = jnp.zeros((1, UNK), jnp.int32)
    start = jnp.int32(0)
    for b in range(BLOCKS):
        size = len_ref[0, b]
        end = start + size
        target = jnp.where((block == b) & (within < size), start + within, target)
        inside = (column >= start) & (column < end)
        first = jnp.where(inside, start, first)
        last = jnp.where(inside, end, last)
        start = end
    pick = (iota((UNK, slots), 0) == target).astype(f32).astype(bf16)
    parts = jnp.concatenate([p.astype(f32) for p in split(inverse)], axis=1).astype(bf16)
    wide = one_pass(pick, parts)
    fold = iota((TILES * BLOCKS, UNK), 0)
    fold = fold - BLOCKS * ((fold >= BLOCKS).astype(jnp.int32) + (fold >= 2 * BLOCKS).astype(jnp.int32))
    spread = (fold == column - first).astype(f32).astype(bf16)
    full = one_pass(wide.astype(bf16), spread)
    row = iota((UNK, UNK), 0)
    return jnp.where((row >= first) & (row < last), full, 0.0)


def encoded(vector, core):
    main = jnp.where(core == 0, vector[:, :LANE], vector[:, REST:])
    rest = jnp.where(core == 0, vector[:, LANE:], vector[:, :REST])
    rows = []
    for p in range(PAIRS):
        a, b = PAIR * p, PAIR * p + 1
        rows.append(jnp.concatenate([main[a : a + 1], main[b : b + 1], rest[a : a + 1], rest[b : b + 1]], axis=1))
    return rows


def decoded(rows, core):
    main = jnp.concatenate([r[:, k * LANE : (k + 1) * LANE] for r in rows for k in range(PAIR)], axis=0)
    rest = jnp.concatenate(
        [r[:, PAIR * LANE + k * REST : PAIR * LANE + (k + 1) * REST] for r in rows for k in range(PAIR)], axis=0
    )
    return jnp.where(
        core == 0, jnp.concatenate([main, rest], axis=1), jnp.concatenate([rest, main], axis=1)
    )


def copies_of(operator_ref, held, sems):
    width = operator_ref.shape[1] // COPIES

    def copy_of(k):
        columns = pl.ds(pl.multiple_of(k * width, LANE), width)
        return pltpu.make_async_copy(operator_ref.at[:, columns], held.at[:, columns], sems.at[k])

    return copy_of


def product(matrix, vector, lifted_ref, copy_of, held, spread, cut_ref, home):
    lifted = nt(vector, matrix)
    lifted_ref[...] = lifted
    turned = lifted.T
    for s in range(SYS):
        spread[s] = jnp.broadcast_to(turned[:, s : s + 1], (UNK, LANE))
    low = iota((1, LANE), 1) < REST

    def one(step, carry):
        totals = [[[None] * TILES for _ in range(SYS)] for _ in range(TOGETHER)]
        base = pl.multiple_of(step * (TOGETHER * NC * UNK), LANE)
        for j in range(UNK // 8):
            for s in range(SYS):
                v = spread[s, 8 * j : 8 * j + 8, :]
                for g in range(TOGETHER):
                    for k in range(TILES):
                        term = held[8 * j : 8 * j + 8, pl.ds(base + (g * TILES + k) * LANE, LANE)] * v
                        totals[g][s][k] = term if j == 0 else totals[g][s][k] + term
        for g in range(TOGETHER):
            z = step * TOGETHER + g
            sums = [[jnp.sum(totals[g][s][k], axis=0, keepdims=True) for k in range(TILES)] for s in range(SYS)]
            for p in range(PAIRS):
                a, b = sums[PAIR * p], sums[PAIR * p + 1]
                lo = jnp.where(low, a[1], pltpu.roll(b[1], REST, 1))
                hi = jnp.where(low, pltpu.roll(a[1], REST, 1), b[1])
                for c, row in ((0, (a[0], b[0], lo)), (1, (a[2], b[2], hi))):
                    for k in range(TILES):
                        cut_ref[*home(p, z, c), :, k * LANE : (k + 1) * LANE] = row[k]
        return carry

    if copy_of is None:
        lax.fori_loop(0, NZ // TOGETHER, one, 0)
        return
    per = NZ // COPIES // TOGETHER

    def chunk(k, carry):
        copy_of(k).wait()
        return lax.fori_loop(k * per, (k + 1) * per, one, carry)

    lax.fori_loop(0, COPIES, chunk, 0)


def first_kernel(
    len_hbm, inverse_hbm, residual_hbm, iterate_hbm, operator_hbm,
    cut_ref, matrix_ref, lifted_ref, residual_ref, iterate_ref, held,
    spread, sems, lengths, inverse, small_sems,
):
    small = [
        pltpu.make_async_copy(source, target, small_sems.at[k])
        for k, (source, target) in enumerate(
            ((len_hbm, lengths), (inverse_hbm, inverse), (residual_hbm, residual_ref), (iterate_hbm, iterate_ref))
        )
    ]
    for copy in small:
        copy.start()
    copy_of = copies_of(operator_hbm, held, sems)
    copy_of(0).start()
    for copy in small:
        copy.wait()
    for k in range(1, COPIES):
        copy_of(k).start()
    residual = residual_ref[...]
    matrix = preconditioner(lengths, inverse[...])
    product(matrix, residual, lifted_ref, copy_of, held, spread, cut_ref, lambda p, z, c: (z, c * (PAIRS) + p))
    matrix_ref[...] = matrix


def forward_kernel(arrived_ref, sent_ref):
    rows = jnp.sum(arrived_ref[...], axis=0)
    pairs = PAIRS
    for k in range(NX * NC * NY):
        c = k // NY % NC
        sent_ref[k] = rows[c * pairs : (c + 1) * pairs]


def second_kernel(
    arrived_ref, matrix_ref, residual_ref, held, cut_ref, mapped_ref, lifted_ref, spread
):
    core, x = lax.axis_index("c"), lax.axis_index("x")
    total = None
    for k in range(NX * NC):
        part = arrived_ref[k * NY + x]
        total = part if total is None else total + part
    mapped = decoded([total[p] for p in range(PAIRS)], core)
    matrix = matrix_ref[...]

    def home(p, z, c):
        row = p * NH + lax.div(z, NL)
        x = lax.div(row, EACH)
        return (x * NL + lax.rem(z, NL)) * NC + c, row - x * EACH

    product(matrix, mapped, lifted_ref, None, held, spread, cut_ref, home)
    step = lax.axis_index("zh")
    for e, vector in enumerate((mapped, residual_ref[...])):
        extra = encoded(vector, core)
        for to in range(NX):
            row = jnp.zeros((1, WIDE), f32)
            for p in range(PAIRS):
                at = p * NH + step - to * EACH
                row = jnp.where((at >= 0) & (at < EACH), extra[p], row)
            for k in range(NL * NC):
                cut_ref[to * NL * NC + k, EACH + e] = row
    mapped_ref[...] = mapped


def share_kernel(arrived_ref, sent_ref):
    near = jnp.sum(arrived_ref[:, :EACH], axis=0)
    own = (lax.axis_index("y") * NL + lax.axis_index("zl")) * NC + lax.axis_index("c")
    rows = [near[j] for j in range(EACH)] + [arrived_ref[own, EACH], arrived_ref[own, EACH + 1]]
    for k in range(NH):
        for j, row in enumerate(rows):
            for i in range(TILES):
                sent_ref[k, j * TILES + i : j * TILES + i + 1, :] = row[:, i * LANE : (i + 1) * LANE]


def dots_kernel(far_ref, sent_ref):
    base = lax.axis_index("x") * EACH
    first = lax.div(base, NH)
    step = lax.axis_index("zh")
    mine = jnp.zeros((1, WIDE), f32)
    terms = [jnp.zeros((1, WIDE), f32)] * (2 * DOTS)
    total = far_ref[0]
    for k in range(1, NH):
        total = total + far_ref[k]

    def row(block, j):
        return jnp.concatenate([block[j * TILES + i : j * TILES + i + 1] for i in range(TILES)], axis=1)

    for j in range(EACH):
        t = row(total, j)
        h = lax.rem(base + j, NH)
        mine = jnp.where(h == step, t, mine)
        source = far_ref[h]
        m, r = row(source, EACH), row(source, EACH + 1)
        same = lax.div(base + j, NH) == first
        for d, term in enumerate((r * r, r * m, m * m, t * r, t * m, t * t)):
            terms[d] = terms[d] + jnp.where(same, term, 0.0)
            terms[DOTS + d] = terms[DOTS + d] + jnp.where(same, 0.0, term)
    terms = jnp.concatenate(terms, axis=0)
    main, other, shared = (terms[:, k * LANE : (k + 1) * LANE] for k in range(TILES))
    low = iota(shared.shape, 1) < REST
    main = main + jnp.where(low, shared, 0.0)
    other = other + jnp.where(low, 0.0, shared)
    column = jnp.sum(
        jnp.concatenate([main[:DOTS], other[:DOTS], main[DOTS:], other[DOTS:]], axis=0), axis=1, keepdims=True
    )
    shape = (2 * PAIR * DOTS, LANE)
    place = iota(shape, 0) + first * (PAIR * DOTS)
    line = jnp.sum(jnp.where(place == iota(shape, 1), column, 0.0), axis=0, keepdims=True)
    sent = jnp.concatenate([mine, line], axis=1)
    for k in range(sent_ref.shape[0]):
        sent_ref[k] = sent


def last_kernel(arrived_ref, iterate_ref, residual_ref, mapped_ref, lifted_ref, lifted_two_ref, new_iterate_ref, new_residual_ref):
    core, x = lax.axis_index("c"), lax.axis_index("x")
    totals = jnp.sum(arrived_ref[:, :, WIDE:], axis=0)
    lane = iota((SYS, LANE), 1)
    system = iota((SYS, LANE), 0)
    home = (system // PAIR) * (PAIR * DOTS) + (system % PAIR) * DOTS
    norm_res, curve_one, square_map, mixed_res, mixed_map, square_two = (
        jnp.sum(jnp.where(lane == home + d, totals, 0.0), axis=1, keepdims=True) for d in range(DOTS)
    )
    alpha = norm_res / curve_one
    cross_mid = curve_one - alpha * square_map - alpha * mixed_res + alpha * alpha * mixed_map
    square_mid = square_map - 2.0 * alpha * mixed_map + alpha * alpha * square_two
    omega = cross_mid / square_mid
    mapped, lifted = mapped_ref[...], lifted_ref[...]
    rows = []
    for p in range(PAIRS):
        source = lax.div(p * NH + lax.axis_index("zh"), EACH)
        rows.append(arrived_ref[((source * NL + lax.axis_index("zl")) * NC + core) * NY + x][:, :WIDE])
    mapped_two = decoded(rows, core)
    middle = residual_ref[...] - alpha * mapped
    lifted_mid = lifted - alpha * lifted_two_ref[...]
    new_iterate_ref[...] = iterate_ref[...] + alpha * lifted + omega * lifted_mid
    new_residual_ref[...] = middle - omega * (mapped - alpha * mapped_two)


def exchanged(pieces, axes):
    return lax.all_to_all(pieces, axes, split_axis=0, concat_axis=0, tiled=True)


def body(operator, block_inverse, block_len, iterate, residual):
    def shape(*lengths):
        return jax.ShapeDtypeStruct(lengths, f32)

    hbm = pl.BlockSpec(memory_space=pltpu.HBM)
    small = shape(SYS, UNK)
    scratch = [pltpu.VMEM((SYS, UNK, LANE), f32)]
    params = pltpu.CompilerParams(vmem_limit_bytes=16 << 20)
    light = pltpu.CompilerParams(vmem_limit_bytes=4 << 20)
    inputs = (block_len, block_inverse.reshape(BLOCKS * BLOCKS, BLOCKS), residual, iterate, operator)
    inputs = [pltpu.with_memory_space_constraint(a, pltpu.HBM) for a in inputs]

    cut, matrix, lifted, residual, iterate, held = pl.pallas_call(
        first_kernel,
        out_shape=(shape(NZ, NC * PAIRS, 1, WIDE), shape(UNK, UNK), small, small, small, shape(*operator.shape)),
        in_specs=[hbm] * 5,
        out_specs=[VM] * 6,
        scratch_shapes=[
            *scratch,
            pltpu.SemaphoreType.DMA((COPIES,)),
            pltpu.SMEM((1, BLOCKS), jnp.int32),
            pltpu.VMEM((BLOCKS * BLOCKS, BLOCKS), f32),
            pltpu.SemaphoreType.DMA((4,)),
        ],
        compiler_params=params,
        name="first_product",
    )(*inputs)

    def call(kernel, name, out_shape, *operands):
        return pl.pallas_call(
            kernel,
            out_shape=out_shape,
            in_specs=[VM] * len(operands),
            out_specs=jax.tree.map(lambda _: VM, out_shape),
            compiler_params=light,
            name=name,
        )(*operands)

    sent = call(forward_kernel, "forward", shape(NX * NC * NY, PAIRS, 1, WIDE), exchanged(cut, Z))
    arrived = exchanged(sent, ("x", "c", "y"))

    cut, mapped, lifted_two = pl.pallas_call(
        second_kernel,
        out_shape=(shape(NX * NL * NC, EACH + 2, 1, WIDE), small, small),
        in_specs=[VM] * 4,
        out_specs=[VM] * 3,
        scratch_shapes=scratch,
        compiler_params=params,
        name="second_product",
    )(arrived, matrix, residual, held)

    sent = call(share_kernel, "share", shape(NH, (EACH + 2) * TILES, LANE), exchanged(cut, ("x", "zl", "c")))
    sent = call(dots_kernel, "dots", shape(NX * NL * NC * NY, 1, WIDE + LANE), exchanged(sent, "zh"))
    arrived = exchanged(sent, ("x", "zl", "c", "y"))
    return call(last_kernel, "update", (small, small), arrived, iterate, residual, mapped, lifted, lifted_two)


def solution(mesh):
    torus = Mesh(mesh.devices.reshape(NX, NH, NL, NC, NY), (*ROWS, "y"))
    placed = (P(ROWS, "y"), P(ROWS, None, None), P(ROWS, None), P(None, ROWS), P(None, ROWS))
    return jax.shard_map(
        body, mesh=torus, in_specs=placed, out_specs=(P(None, ROWS), P(None, ROWS)), check_vma=False
    )
```

```python
import functools

import jax
import jax.numpy as jnp
from jax import lax
from jax.experimental import pallas as pl
from jax.experimental.pallas import tpu as pltpu
from jax.sharding import Mesh
from jax.sharding import PartitionSpec as P

Z = ("zh", "zl")
ROWS = ("x", *Z, "c")
NX, NH, NL, NC, NY = 4, 8, 2, 2, 4
NZ = NH * NL
SYS, UNK, LANE = 6, 192, 128
REST = UNK - LANE
PAIR = 2
WIDE = PAIR * UNK
TILES = WIDE // LANE
BLOCKS = 24
COPIES = 4
TOGETHER = 2
DOTS = 6
PAIRS = SYS // PAIR
EACH = PAIRS * NH // NX

highest = lax.Precision.HIGHEST
f32, bf16 = jnp.float32, jnp.bfloat16
VM = pl.BlockSpec(memory_space=pltpu.VMEM)


def iota(shape, dim):
    return lax.broadcasted_iota(jnp.int32, shape, dim)


def split(value):
    high = value.astype(bf16)
    left = value - high.astype(f32)
    middle = left.astype(bf16)
    return high, middle, (left - middle.astype(f32)).astype(bf16)


def one_pass(a, b):
    return jnp.dot(a, b, preferred_element_type=f32)


def nt(vector, matrix):
    padded = jnp.concatenate([vector, jnp.zeros((8 - SYS, UNK), f32)], axis=0)
    rows = jnp.concatenate([p.astype(f32) for p in split(padded)], axis=0).astype(bf16)
    total = None
    for k, part in reversed(list(enumerate(split(matrix)))):
        out = lax.dot_general(
            rows[: 8 * (TILES - k)], part, (((1,), (1,)), ((), ())), preferred_element_type=f32
        )
        for e in reversed(range(TILES - k)):
            piece = out[8 * e : 8 * e + 8]
            total = piece if total is None else total + piece
    return total[:SYS]


def preconditioner(len_ref, inverse):
    slots = BLOCKS * BLOCKS
    slot = iota((1, slots), 1)
    block = slot // BLOCKS
    within = slot - block * BLOCKS
    column = iota((1, UNK), 1)
    target = jnp.full((1, slots), -1, jnp.int32)
    first = jnp.zeros((1, UNK), jnp.int32)
    last = jnp.zeros((1, UNK), jnp.int32)
    start = jnp.int32(0)
    for b in range(BLOCKS):
        size = len_ref[0, b]
        end = start + size
        target = jnp.where((block == b) & (within < size), start + within, target)
        inside = (column >= start) & (column < end)
        first = jnp.where(inside, start, first)
        last = jnp.where(inside, end, last)
        start = end
    pick = (iota((UNK, slots), 0) == target).astype(f32).astype(bf16)
    parts = jnp.concatenate([p.astype(f32) for p in split(inverse)], axis=1).astype(bf16)
    wide = one_pass(pick, parts)
    fold = iota((TILES * BLOCKS, UNK), 0)
    fold = fold - BLOCKS * ((fold >= BLOCKS).astype(jnp.int32) + (fold >= 2 * BLOCKS).astype(jnp.int32))
    spread = (fold == column - first).astype(f32).astype(bf16)
    full = one_pass(wide.astype(bf16), spread)
    row = iota((UNK, UNK), 0)
    return jnp.where((row >= first) & (row < last), full, 0.0)


def encoded(vector, core):
    main = jnp.where(core == 0, vector[:, :LANE], vector[:, REST:])
    rest = jnp.where(core == 0, vector[:, LANE:], vector[:, :REST])
    rows = []
    for p in range(PAIRS):
        a, b = PAIR * p, PAIR * p + 1
        rows.append(jnp.concatenate([main[a : a + 1], main[b : b + 1], rest[a : a + 1], rest[b : b + 1]], axis=1))
    return rows


def decoded(rows, core):
    main = jnp.concatenate([r[:, k * LANE : (k + 1) * LANE] for r in rows for k in range(PAIR)], axis=0)
    rest = jnp.concatenate(
        [r[:, PAIR * LANE + k * REST : PAIR * LANE + (k + 1) * REST] for r in rows for k in range(PAIR)], axis=0
    )
    return jnp.where(
        core == 0, jnp.concatenate([main, rest], axis=1), jnp.concatenate([rest, main], axis=1)
    )


def copies_of(operator_ref, held, sems):
    width = operator_ref.shape[1] // COPIES

    def copy_of(k):
        columns = pl.ds(pl.multiple_of(k * width, LANE), width)
        return pltpu.make_async_copy(operator_ref.at[:, columns], held.at[:, columns], sems.at[k])

    return copy_of


def product(matrix, vector, lifted_ref, copy_of, held, spread, cut_ref, home):
    lifted = nt(vector, matrix)
    lifted_ref[...] = lifted
    turned = lifted.T
    for s in range(SYS):
        spread[s] = jnp.broadcast_to(turned[:, s : s + 1], (UNK, LANE))
    low = iota((1, LANE), 1) < REST

    def one(step, carry):
        totals = [[[None] * TILES for _ in range(SYS)] for _ in range(TOGETHER)]
        base = pl.multiple_of(step * (TOGETHER * NC * UNK), LANE)
        for j in range(UNK // 8):
            for s in range(SYS):
                v = spread[s, 8 * j : 8 * j + 8, :]
                for g in range(TOGETHER):
                    for k in range(TILES):
                        term = held[8 * j : 8 * j + 8, pl.ds(base + (g * TILES + k) * LANE, LANE)] * v
                        totals[g][s][k] = term if j == 0 else totals[g][s][k] + term
        for g in range(TOGETHER):
            z = step * TOGETHER + g
            sums = [[jnp.sum(totals[g][s][k], axis=0, keepdims=True) for k in range(TILES)] for s in range(SYS)]
            for p in range(PAIRS):
                a, b = sums[PAIR * p], sums[PAIR * p + 1]
                lo = jnp.where(low, a[1], pltpu.roll(b[1], REST, 1))
                hi = jnp.where(low, pltpu.roll(a[1], REST, 1), b[1])
                for c, row in ((0, (a[0], b[0], lo)), (1, (a[2], b[2], hi))):
                    for k in range(TILES):
                        cut_ref[*home(p, z, c), :, k * LANE : (k + 1) * LANE] = row[k]
        return carry

    if copy_of is None:
        lax.fori_loop(0, NZ // TOGETHER, one, 0)
        return
    per = NZ // COPIES // TOGETHER

    def chunk(k, carry):
        copy_of(k).wait()
        return lax.fori_loop(k * per, (k + 1) * per, one, carry)

    lax.fori_loop(0, COPIES, chunk, 0)


def first_kernel(
    len_hbm, inverse_hbm, residual_hbm, iterate_hbm, operator_hbm,
    cut_ref, matrix_ref, lifted_ref, residual_ref, iterate_ref, held,
    spread, sems, lengths, inverse, small_sems,
):
    small = [
        pltpu.make_async_copy(source, target, small_sems.at[k])
        for k, (source, target) in enumerate(
            ((len_hbm, lengths), (inverse_hbm, inverse), (residual_hbm, residual_ref), (iterate_hbm, iterate_ref))
        )
    ]
    for copy in small:
        copy.start()
    copy_of = copies_of(operator_hbm, held, sems)
    copy_of(0).start()
    for copy in small:
        copy.wait()
    for k in range(1, COPIES):
        copy_of(k).start()
    residual = residual_ref[...]
    matrix = preconditioner(lengths, inverse[...])
    product(matrix, residual, lifted_ref, copy_of, held, spread, cut_ref, lambda p, z, c: (z, c * (PAIRS) + p))
    matrix_ref[...] = matrix


def forward_kernel(arrived_ref, sent_ref):
    rows = jnp.sum(arrived_ref[...], axis=0)
    pairs = PAIRS
    for k in range(NX * NC * NY):
        c = k // NY % NC
        sent_ref[k] = rows[c * pairs : (c + 1) * pairs]


def second_kernel(
    arrived_ref, matrix_ref, residual_ref, held, cut_ref, mapped_ref, lifted_ref, spread
):
    core, x = lax.axis_index("c"), lax.axis_index("x")
    total = None
    for k in range(NX * NC):
        part = arrived_ref[k * NY + x]
        total = part if total is None else total + part
    mapped = decoded([total[p] for p in range(PAIRS)], core)
    matrix = matrix_ref[...]
    far = lax.div(lax.axis_index("zh"), NH // 2)

    def home(p, z, c):
        row = p * NH + lax.div(z, NL)
        x = lax.div(row, EACH)
        return (x * NL + lax.rem(z, NL)) * NC + lax.rem(c + far, NC), row - x * EACH

    product(matrix, mapped, lifted_ref, None, held, spread, cut_ref, home)
    step = lax.axis_index("zh")
    for e, vector in enumerate((mapped, residual_ref[...])):
        extra = encoded(vector, core)
        for to in range(NX):
            row = jnp.zeros((1, WIDE), f32)
            for p in range(PAIRS):
                at = p * NH + step - to * EACH
                row = jnp.where((at >= 0) & (at < EACH), extra[p], row)
            for k in range(NL * NC):
                cut_ref[to * NL * NC + k, EACH + e] = row
    mapped_ref[...] = mapped


def share_kernel(arrived_ref, sent_ref):
    near = jnp.sum(arrived_ref[:, :EACH], axis=0)
    own = (lax.axis_index("y") * NL + lax.axis_index("zl")) * NC + turned_core()
    rows = [near[j] for j in range(EACH)] + [arrived_ref[own, EACH], arrived_ref[own, EACH + 1]]
    for k in range(NH):
        for j, row in enumerate(rows):
            for i in range(TILES):
                sent_ref[k, j * TILES + i : j * TILES + i + 1, :] = row[:, i * LANE : (i + 1) * LANE]


def dots_kernel(far_ref, sent_ref):
    base = lax.axis_index("x") * EACH
    first = lax.div(base, NH)
    step = lax.axis_index("zh")
    mine = jnp.zeros((1, WIDE), f32)
    terms = [jnp.zeros((1, WIDE), f32)] * (2 * DOTS)
    total = far_ref[0]
    for k in range(1, NH):
        total = total + far_ref[k]

    def row(block, j):
        return jnp.concatenate([block[j * TILES + i : j * TILES + i + 1] for i in range(TILES)], axis=1)

    for j in range(EACH):
        t = row(total, j)
        h = lax.rem(base + j, NH)
        mine = jnp.where(h == step, t, mine)
        source = far_ref[h]
        m, r = row(source, EACH), row(source, EACH + 1)
        same = lax.div(base + j, NH) == first
        for d, term in enumerate((r * r, r * m, m * m, t * r, t * m, t * t)):
            terms[d] = terms[d] + jnp.where(same, term, 0.0)
            terms[DOTS + d] = terms[DOTS + d] + jnp.where(same, 0.0, term)
    terms = jnp.concatenate(terms, axis=0)
    main, other, shared = (terms[:, k * LANE : (k + 1) * LANE] for k in range(TILES))
    low = iota(shared.shape, 1) < REST
    main = main + jnp.where(low, shared, 0.0)
    other = other + jnp.where(low, 0.0, shared)
    column = jnp.sum(
        jnp.concatenate([main[:DOTS], other[:DOTS], main[DOTS:], other[DOTS:]], axis=0), axis=1, keepdims=True
    )
    shape = (2 * PAIR * DOTS, LANE)
    place = iota(shape, 0) + first * (PAIR * DOTS)
    line = jnp.sum(jnp.where(place == iota(shape, 1), column, 0.0), axis=0, keepdims=True)
    sent = jnp.concatenate([mine, line], axis=1)
    for k in range(sent_ref.shape[0]):
        sent_ref[k] = sent


def last_kernel(arrived_ref, iterate_ref, residual_ref, mapped_ref, lifted_ref, lifted_two_ref, new_iterate_ref, new_residual_ref):
    core, x = lax.axis_index("c"), lax.axis_index("x")
    totals = jnp.sum(arrived_ref[:, :, WIDE:], axis=0)
    lane = iota((SYS, LANE), 1)
    system = iota((SYS, LANE), 0)
    home = (system // PAIR) * (PAIR * DOTS) + (system % PAIR) * DOTS
    norm_res, curve_one, square_map, mixed_res, mixed_map, square_two = (
        jnp.sum(jnp.where(lane == home + d, totals, 0.0), axis=1, keepdims=True) for d in range(DOTS)
    )
    alpha = norm_res / curve_one
    cross_mid = curve_one - alpha * square_map - alpha * mixed_res + alpha * alpha * mixed_map
    square_mid = square_map - 2.0 * alpha * mixed_map + alpha * alpha * square_two
    omega = cross_mid / square_mid
    mapped, lifted = mapped_ref[...], lifted_ref[...]
    rows = []
    for p in range(PAIRS):
        source = lax.div(p * NH + lax.axis_index("zh"), EACH)
        rows.append(arrived_ref[((source * NL + lax.axis_index("zl")) * NC + turned_core()) * NY + x][:, :WIDE])
    mapped_two = decoded(rows, core)
    middle = residual_ref[...] - alpha * mapped
    lifted_mid = lifted - alpha * lifted_two_ref[...]
    new_iterate_ref[...] = iterate_ref[...] + alpha * lifted + omega * lifted_mid
    new_residual_ref[...] = middle - omega * (mapped - alpha * mapped_two)


def exchanged(pieces, axes, groups=None):
    return lax.all_to_all(pieces, axes, split_axis=0, concat_axis=0, tiled=True, axis_index_groups=groups)


def crossed(length):
    return [[k * NC + (g + 2 * k // length) % NC for k in range(length)] for g in range(NC)]


def turned_core():
    return lax.rem(lax.axis_index("c") + lax.div(lax.axis_index("zh"), NH // 2), NC)


def body(operator, block_inverse, block_len, iterate, residual):
    def shape(*lengths):
        return jax.ShapeDtypeStruct(lengths, f32)

    hbm = pl.BlockSpec(memory_space=pltpu.HBM)
    small = shape(SYS, UNK)
    scratch = [pltpu.VMEM((SYS, UNK, LANE), f32)]
    params = pltpu.CompilerParams(vmem_limit_bytes=16 << 20)
    light = pltpu.CompilerParams(vmem_limit_bytes=4 << 20)
    inputs = (block_len, block_inverse.reshape(BLOCKS * BLOCKS, BLOCKS), residual, iterate, operator)
    inputs = [pltpu.with_memory_space_constraint(a, pltpu.HBM) for a in inputs]

    cut, matrix, lifted, residual, iterate, held = pl.pallas_call(
        first_kernel,
        out_shape=(shape(NZ, NC * PAIRS, 1, WIDE), shape(UNK, UNK), small, small, small, shape(*operator.shape)),
        in_specs=[hbm] * 5,
        out_specs=[VM] * 6,
        scratch_shapes=[
            *scratch,
            pltpu.SemaphoreType.DMA((COPIES,)),
            pltpu.SMEM((1, BLOCKS), jnp.int32),
            pltpu.VMEM((BLOCKS * BLOCKS, BLOCKS), f32),
            pltpu.SemaphoreType.DMA((4,)),
        ],
        compiler_params=params,
        name="first_product",
    )(*inputs)

    def call(kernel, name, out_shape, *operands):
        return pl.pallas_call(
            kernel,
            out_shape=out_shape,
            in_specs=[VM] * len(operands),
            out_specs=jax.tree.map(lambda _: VM, out_shape),
            compiler_params=light,
            name=name,
        )(*operands)

    sent = call(forward_kernel, "forward", shape(NX * NC * NY, PAIRS, 1, WIDE), exchanged(cut, (*Z, "c"), crossed(NZ)))
    arrived = exchanged(sent, ("x", "c", "y"))

    cut, mapped, lifted_two = pl.pallas_call(
        second_kernel,
        out_shape=(shape(NX * NL * NC, EACH + 2, 1, WIDE), small, small),
        in_specs=[VM] * 4,
        out_specs=[VM] * 3,
        scratch_shapes=scratch,
        compiler_params=params,
        name="second_product",
    )(arrived, matrix, residual, held)

    sent = call(share_kernel, "share", shape(NH, (EACH + 2) * TILES, LANE), exchanged(cut, ("x", "zl", "c")))
    sent = call(dots_kernel, "dots", shape(NX * NL * NC * NY, 1, WIDE + LANE), exchanged(sent, ("zh", "c"), crossed(NH)))
    arrived = exchanged(sent, ("x", "zl", "c", "y"))
    return call(last_kernel, "update", (small, small), arrived, iterate, residual, mapped, lifted, lifted_two)


def solution(mesh):
    torus = Mesh(mesh.devices.reshape(NX, NH, NL, NC, NY), (*ROWS, "y"))
    placed = (P(ROWS, "y"), P(ROWS, None, None), P(ROWS, None), P(None, ROWS), P(None, ROWS))
    return jax.shard_map(
        body, mesh=torus, in_specs=placed, out_specs=(P(None, ROWS), P(None, ROWS)), check_vma=False
    )
```

```python
import functools

import jax
import jax.numpy as jnp
from jax import lax
from jax.experimental import pallas as pl
from jax.experimental.pallas import tpu as pltpu
from jax.sharding import Mesh
from jax.sharding import PartitionSpec as P

Z = ("zh", "zl")
ROWS = ("x", *Z, "c")
NX, NH, NL, NC, NY = 4, 8, 2, 2, 4
NZ = NH * NL
SYS, UNK, LANE = 6, 192, 128
REST = UNK - LANE
PAIR = 2
WIDE = PAIR * UNK
TILES = WIDE // LANE
BLOCKS = 24
COPIES = 4
TOGETHER = 2
DOTS = 6
PAIRS = SYS // PAIR
EACH = PAIRS * NH // NX

highest = lax.Precision.HIGHEST
f32, bf16 = jnp.float32, jnp.bfloat16
VM = pl.BlockSpec(memory_space=pltpu.VMEM)


def iota(shape, dim):
    return lax.broadcasted_iota(jnp.int32, shape, dim)


def split(value):
    high = value.astype(bf16)
    left = value - high.astype(f32)
    middle = left.astype(bf16)
    return high, middle, (left - middle.astype(f32)).astype(bf16)


def one_pass(a, b):
    return jnp.dot(a, b, preferred_element_type=f32)


def nt(vector, matrix):
    padded = jnp.concatenate([vector, jnp.zeros((8 - SYS, UNK), f32)], axis=0)
    rows = jnp.concatenate([p.astype(f32) for p in split(padded)], axis=0).astype(bf16)
    total = None
    for k, part in reversed(list(enumerate(split(matrix)))):
        out = lax.dot_general(
            rows[: 8 * (TILES - k)], part, (((1,), (1,)), ((), ())), preferred_element_type=f32
        )
        for e in reversed(range(TILES - k)):
            piece = out[8 * e : 8 * e + 8]
            total = piece if total is None else total + piece
    return total[:SYS]


def preconditioner(len_ref, inverse):
    slots = BLOCKS * BLOCKS
    slot = iota((1, slots), 1)
    block = slot // BLOCKS
    within = slot - block * BLOCKS
    column = iota((1, UNK), 1)
    target = jnp.full((1, slots), -1, jnp.int32)
    first = jnp.zeros((1, UNK), jnp.int32)
    last = jnp.zeros((1, UNK), jnp.int32)
    start = jnp.int32(0)
    for b in range(BLOCKS):
        size = len_ref[0, b]
        end = start + size
        target = jnp.where((block == b) & (within < size), start + within, target)
        inside = (column >= start) & (column < end)
        first = jnp.where(inside, start, first)
        last = jnp.where(inside, end, last)
        start = end
    pick = (iota((UNK, slots), 0) == target).astype(f32).astype(bf16)
    parts = jnp.concatenate([p.astype(f32) for p in split(inverse)], axis=1).astype(bf16)
    wide = one_pass(pick, parts)
    fold = iota((TILES * BLOCKS, UNK), 0)
    fold = fold - BLOCKS * ((fold >= BLOCKS).astype(jnp.int32) + (fold >= 2 * BLOCKS).astype(jnp.int32))
    spread = (fold == column - first).astype(f32).astype(bf16)
    full = one_pass(wide.astype(bf16), spread)
    row = iota((UNK, UNK), 0)
    return jnp.where((row >= first) & (row < last), full, 0.0)


def encoded(vector, core):
    main = jnp.where(core == 0, vector[:, :LANE], vector[:, REST:])
    rest = jnp.where(core == 0, vector[:, LANE:], vector[:, :REST])
    rows = []
    for p in range(PAIRS):
        a, b = PAIR * p, PAIR * p + 1
        rows.append(jnp.concatenate([main[a : a + 1], main[b : b + 1], rest[a : a + 1], rest[b : b + 1]], axis=1))
    return rows


def decoded(rows, core):
    main = jnp.concatenate([r[:, k * LANE : (k + 1) * LANE] for r in rows for k in range(PAIR)], axis=0)
    rest = jnp.concatenate(
        [r[:, PAIR * LANE + k * REST : PAIR * LANE + (k + 1) * REST] for r in rows for k in range(PAIR)], axis=0
    )
    return jnp.where(
        core == 0, jnp.concatenate([main, rest], axis=1), jnp.concatenate([rest, main], axis=1)
    )


def copies_of(operator_ref, held, sems):
    width = operator_ref.shape[1] // COPIES

    def copy_of(k):
        columns = pl.ds(pl.multiple_of(k * width, LANE), width)
        return pltpu.make_async_copy(operator_ref.at[:, columns], held.at[:, columns], sems.at[k])

    return copy_of


def product(matrix, vector, lifted_ref, copy_of, held, spread, cut_ref, home):
    lifted = nt(vector, matrix)
    lifted_ref[...] = lifted
    turned = lifted.T
    for s in range(SYS):
        spread[s] = jnp.broadcast_to(turned[:, s : s + 1], (UNK, LANE))
    low = iota((1, LANE), 1) < REST

    def one(step, carry):
        totals = [[[None] * TILES for _ in range(SYS)] for _ in range(TOGETHER)]
        base = pl.multiple_of(step * (TOGETHER * NC * UNK), LANE)
        for j in range(UNK // 8):
            for s in range(SYS):
                v = spread[s, 8 * j : 8 * j + 8, :]
                for g in range(TOGETHER):
                    for k in range(TILES):
                        term = held[8 * j : 8 * j + 8, pl.ds(base + (g * TILES + k) * LANE, LANE)] * v
                        totals[g][s][k] = term if j == 0 else totals[g][s][k] + term
        for g in range(TOGETHER):
            z = step * TOGETHER + g
            sums = [[jnp.sum(totals[g][s][k], axis=0, keepdims=True) for k in range(TILES)] for s in range(SYS)]
            for p in range(PAIRS):
                a, b = sums[PAIR * p], sums[PAIR * p + 1]
                lo = jnp.where(low, a[1], pltpu.roll(b[1], REST, 1))
                hi = jnp.where(low, pltpu.roll(a[1], REST, 1), b[1])
                for c, row in ((0, (a[0], b[0], lo)), (1, (a[2], b[2], hi))):
                    for k in range(TILES):
                        cut_ref[*home(p, z, c), :, k * LANE : (k + 1) * LANE] = row[k]
        return carry

    if copy_of is None:
        lax.fori_loop(0, NZ // TOGETHER, one, 0)
        return
    per = NZ // COPIES // TOGETHER

    def chunk(k, carry):
        copy_of(k).wait()
        return lax.fori_loop(k * per, (k + 1) * per, one, carry)

    lax.fori_loop(0, COPIES, chunk, 0)


def first_kernel(
    len_hbm, inverse_hbm, residual_hbm, iterate_hbm, operator_hbm,
    cut_ref, matrix_ref, lifted_ref, residual_ref, iterate_ref, held,
    spread, sems, lengths, inverse, small_sems,
):
    small = [
        pltpu.make_async_copy(source, target, small_sems.at[k])
        for k, (source, target) in enumerate(
            ((len_hbm, lengths), (inverse_hbm, inverse), (residual_hbm, residual_ref), (iterate_hbm, iterate_ref))
        )
    ]
    for copy in small:
        copy.start()
    copy_of = copies_of(operator_hbm, held, sems)
    copy_of(0).start()
    for copy in small:
        copy.wait()
    for k in range(1, COPIES):
        copy_of(k).start()
    residual = residual_ref[...]
    matrix = preconditioner(lengths, inverse[...])
    product(matrix, residual, lifted_ref, copy_of, held, spread, cut_ref, lambda p, z, c: (z, c * (PAIRS) + p))
    matrix_ref[...] = matrix


def forward_kernel(arrived_ref, sent_ref):
    rows = jnp.sum(arrived_ref[...], axis=0)
    pairs = PAIRS
    for k in range(NX * NC * NY):
        c = k // NY % NC
        sent_ref[k] = rows[c * pairs : (c + 1) * pairs]


def second_kernel(
    arrived_ref, matrix_ref, residual_ref, held, cut_ref, mapped_ref, lifted_ref, spread
):
    core, x = lax.axis_index("c"), lax.axis_index("x")
    total = None
    for k in range(NX * NC):
        part = arrived_ref[k * NY + x]
        total = part if total is None else total + part
    mapped = decoded([total[p] for p in range(PAIRS)], core)
    matrix = matrix_ref[...]
    far = lax.div(lax.axis_index("zh"), NH // 2)

    def home(p, z, c):
        row = p * NH + lax.div(z, NL)
        x = lax.div(row, EACH)
        return (x * NL + lax.rem(z, NL)) * NC + lax.rem(c + far, NC), row - x * EACH

    product(matrix, mapped, lifted_ref, None, held, spread, cut_ref, home)
    step = lax.axis_index("zh")
    for e, vector in enumerate((mapped, residual_ref[...])):
        extra = encoded(vector, core)
        for to in range(NX):
            row = jnp.zeros((1, WIDE), f32)
            for p in range(PAIRS):
                at = p * NH + step - to * EACH
                row = jnp.where((at >= 0) & (at < EACH), extra[p], row)
            for k in range(NL * NC):
                cut_ref[to * NL * NC + k, EACH + e] = row
    mapped_ref[...] = mapped


def share_kernel(arrived_ref, sent_ref):
    near = jnp.sum(arrived_ref[:, :EACH], axis=0)
    own = (lax.axis_index("y") * NL + lax.axis_index("zl")) * NC + turned_core()
    rows = [near[j] for j in range(EACH)] + [arrived_ref[own, EACH], arrived_ref[own, EACH + 1]]
    for k in range(NH):
        for j, row in enumerate(rows):
            for i in range(TILES):
                sent_ref[k, j * TILES + i : j * TILES + i + 1, :] = row[:, i * LANE : (i + 1) * LANE]


def dots_kernel(far_ref, sent_ref):
    base = lax.axis_index("x") * EACH
    first = lax.div(base, NH)
    step = lax.axis_index("zh")
    mine = jnp.zeros((1, WIDE), f32)
    terms = [jnp.zeros((1, WIDE), f32)] * (2 * DOTS)
    total = far_ref[0]
    for k in range(1, NH):
        total = total + far_ref[k]

    def row(block, j):
        return jnp.concatenate([block[j * TILES + i : j * TILES + i + 1] for i in range(TILES)], axis=1)

    for j in range(EACH):
        t = row(total, j)
        h = lax.rem(base + j, NH)
        mine = jnp.where(h == step, t, mine)
        source = far_ref[h]
        m, r = row(source, EACH), row(source, EACH + 1)
        same = lax.div(base + j, NH) == first
        for d, term in enumerate((r * r, r * m, m * m, t * r, t * m, t * t)):
            terms[d] = terms[d] + jnp.where(same, term, 0.0)
            terms[DOTS + d] = terms[DOTS + d] + jnp.where(same, 0.0, term)
    terms = jnp.concatenate(terms, axis=0)
    main, other, shared = (terms[:, k * LANE : (k + 1) * LANE] for k in range(TILES))
    low = iota(shared.shape, 1) < REST
    main = main + jnp.where(low, shared, 0.0)
    other = other + jnp.where(low, 0.0, shared)
    column = jnp.sum(
        jnp.concatenate([main[:DOTS], other[:DOTS], main[DOTS:], other[DOTS:]], axis=0), axis=1, keepdims=True
    )
    shape = (2 * PAIR * DOTS, LANE)
    place = iota(shape, 0) + first * (PAIR * DOTS)
    line = jnp.sum(jnp.where(place == iota(shape, 1), column, 0.0), axis=0, keepdims=True)
    sent = jnp.concatenate([mine, line], axis=1)
    for k in range(sent_ref.shape[0]):
        sent_ref[k] = sent


def last_kernel(arrived_ref, iterate_ref, residual_ref, mapped_ref, lifted_ref, lifted_two_ref, new_iterate_ref, new_residual_ref):
    core, x = lax.axis_index("c"), lax.axis_index("x")
    totals = jnp.sum(arrived_ref[:, :, WIDE:], axis=0)
    lane = iota((SYS, LANE), 1)
    system = iota((SYS, LANE), 0)
    home = (system // PAIR) * (PAIR * DOTS) + (system % PAIR) * DOTS
    norm_res, curve_one, square_map, mixed_res, mixed_map, square_two = (
        jnp.sum(jnp.where(lane == home + d, totals, 0.0), axis=1, keepdims=True) for d in range(DOTS)
    )
    alpha = norm_res / curve_one
    cross_mid = curve_one - alpha * square_map - alpha * mixed_res + alpha * alpha * mixed_map
    square_mid = square_map - 2.0 * alpha * mixed_map + alpha * alpha * square_two
    omega = cross_mid / square_mid
    mapped, lifted = mapped_ref[...], lifted_ref[...]
    rows = []
    for p in range(PAIRS):
        source = lax.div(p * NH + lax.axis_index("zh"), EACH)
        rows.append(arrived_ref[((source * NL + lax.axis_index("zl")) * NC + turned_core()) * NY + x][:, :WIDE])
    mapped_two = decoded(rows, core)
    middle = residual_ref[...] - alpha * mapped
    lifted_mid = lifted - alpha * lifted_two_ref[...]
    new_iterate_ref[...] = iterate_ref[...] + alpha * lifted + omega * lifted_mid
    new_residual_ref[...] = middle - omega * (mapped - alpha * mapped_two)


def exchanged(pieces, axes, groups=None):
    return lax.all_to_all(pieces, axes, split_axis=0, concat_axis=0, tiled=True, axis_index_groups=groups)


def crossed(length):
    return [[k * NC + (g + 2 * k // length) % NC for k in range(length)] for g in range(NC)]


def turned_core():
    return lax.rem(lax.axis_index("c") + lax.div(lax.axis_index("zh"), NH // 2), NC)


def body(operator, block_inverse, block_len, iterate, residual):
    def shape(*lengths):
        return jax.ShapeDtypeStruct(lengths, f32)

    hbm = pl.BlockSpec(memory_space=pltpu.HBM)
    small = shape(SYS, UNK)
    scratch = [pltpu.VMEM((SYS, UNK, LANE), f32)]
    params = pltpu.CompilerParams(vmem_limit_bytes=16 << 20)
    light = pltpu.CompilerParams(vmem_limit_bytes=4 << 20)
    inputs = (block_len, block_inverse.reshape(BLOCKS * BLOCKS, BLOCKS), residual, iterate, operator)
    inputs = [pltpu.with_memory_space_constraint(a, pltpu.HBM) for a in inputs]

    cut, matrix, lifted, residual, iterate, held = pl.pallas_call(
        first_kernel,
        out_shape=(shape(NZ, NC * PAIRS, 1, WIDE), shape(UNK, UNK), small, small, small, shape(*operator.shape)),
        in_specs=[hbm] * 5,
        out_specs=[VM] * 6,
        scratch_shapes=[
            *scratch,
            pltpu.SemaphoreType.DMA((COPIES,)),
            pltpu.SMEM((1, BLOCKS), jnp.int32),
            pltpu.VMEM((BLOCKS * BLOCKS, BLOCKS), f32),
            pltpu.SemaphoreType.DMA((4,)),
        ],
        compiler_params=params,
        name="first_product",
    )(*inputs)

    def call(kernel, name, out_shape, *operands):
        return pl.pallas_call(
            kernel,
            out_shape=out_shape,
            in_specs=[VM] * len(operands),
            out_specs=jax.tree.map(lambda _: VM, out_shape),
            compiler_params=light,
            name=name,
        )(*operands)

    sent = call(forward_kernel, "forward", shape(NX * NC * NY, PAIRS, 1, WIDE), exchanged(cut, Z))
    arrived = exchanged(sent, ("x", "c", "y"))

    cut, mapped, lifted_two = pl.pallas_call(
        second_kernel,
        out_shape=(shape(NX * NL * NC, EACH + 2, 1, WIDE), small, small),
        in_specs=[VM] * 4,
        out_specs=[VM] * 3,
        scratch_shapes=scratch,
        compiler_params=params,
        name="second_product",
    )(arrived, matrix, residual, held)

    sent = call(share_kernel, "share", shape(NH, (EACH + 2) * TILES, LANE), exchanged(cut, ("x", "zl", "c")))
    sent = call(dots_kernel, "dots", shape(NX * NL * NC * NY, 1, WIDE + LANE), exchanged(sent, ("zh", "c"), crossed(NH)))
    arrived = exchanged(sent, ("x", "zl", "c", "y"))
    return call(last_kernel, "update", (small, small), arrived, iterate, residual, mapped, lifted, lifted_two)


def solution(mesh):
    torus = Mesh(mesh.devices.reshape(NX, NH, NL, NC, NY), (*ROWS, "y"))
    placed = (P(ROWS, "y"), P(ROWS, None, None), P(ROWS, None), P(None, ROWS), P(None, ROWS))
    return jax.shard_map(
        body, mesh=torus, in_specs=placed, out_specs=(P(None, ROWS), P(None, ROWS)), check_vma=False
    )
```

```python
import functools

import jax
import jax.numpy as jnp
from jax import lax
from jax.experimental import pallas as pl
from jax.experimental.pallas import tpu as pltpu
from jax.sharding import Mesh
from jax.sharding import PartitionSpec as P

Z = ("zh", "zl")
ROWS = ("x", *Z, "c")
NX, NH, NL, NC, NY = 4, 8, 2, 2, 4
NZ = NH * NL
SYS, UNK, LANE = 6, 192, 128
REST = UNK - LANE
PAIR = 2
WIDE = PAIR * UNK
TILES = WIDE // LANE
BLOCKS = 24
COPIES = 4
TOGETHER = 2
DOTS = 6
PAIRS = SYS // PAIR
EACH = PAIRS * NH // NX

highest = lax.Precision.HIGHEST
f32, bf16 = jnp.float32, jnp.bfloat16
VM = pl.BlockSpec(memory_space=pltpu.VMEM)


def iota(shape, dim):
    return lax.broadcasted_iota(jnp.int32, shape, dim)


def split(value):
    high = value.astype(bf16)
    left = value - high.astype(f32)
    middle = left.astype(bf16)
    return high, middle, (left - middle.astype(f32)).astype(bf16)


def one_pass(a, b):
    return jnp.dot(a, b, preferred_element_type=f32)


def nt(vector, matrix):
    padded = jnp.concatenate([vector, jnp.zeros((8 - SYS, UNK), f32)], axis=0)
    rows = jnp.concatenate([p.astype(f32) for p in split(padded)], axis=0).astype(bf16)
    total = None
    for k, part in reversed(list(enumerate(split(matrix)))):
        out = lax.dot_general(
            rows[: 8 * (TILES - k)], part, (((1,), (1,)), ((), ())), preferred_element_type=f32
        )
        for e in reversed(range(TILES - k)):
            piece = out[8 * e : 8 * e + 8]
            total = piece if total is None else total + piece
    return total[:SYS]


def preconditioner(len_ref, inverse):
    slots = BLOCKS * BLOCKS
    slot = iota((1, slots), 1)
    block = slot // BLOCKS
    within = slot - block * BLOCKS
    column = iota((1, UNK), 1)
    target = jnp.full((1, slots), -1, jnp.int32)
    first = jnp.zeros((1, UNK), jnp.int32)
    last = jnp.zeros((1, UNK), jnp.int32)
    start = jnp.int32(0)
    for b in range(BLOCKS):
        size = len_ref[0, b]
        end = start + size
        target = jnp.where((block == b) & (within < size), start + within, target)
        inside = (column >= start) & (column < end)
        first = jnp.where(inside, start, first)
        last = jnp.where(inside, end, last)
        start = end
    pick = (iota((UNK, slots), 0) == target).astype(f32).astype(bf16)
    parts = jnp.concatenate([p.astype(f32) for p in split(inverse)], axis=1).astype(bf16)
    wide = one_pass(pick, parts)
    fold = iota((TILES * BLOCKS, UNK), 0)
    fold = fold - BLOCKS * ((fold >= BLOCKS).astype(jnp.int32) + (fold >= 2 * BLOCKS).astype(jnp.int32))
    spread = (fold == column - first).astype(f32).astype(bf16)
    full = one_pass(wide.astype(bf16), spread)
    row = iota((UNK, UNK), 0)
    return jnp.where((row >= first) & (row < last), full, 0.0)


def encoded(vector, core):
    main = jnp.where(core == 0, vector[:, :LANE], vector[:, REST:])
    rest = jnp.where(core == 0, vector[:, LANE:], vector[:, :REST])
    rows = []
    for p in range(PAIRS):
        a, b = PAIR * p, PAIR * p + 1
        rows.append(jnp.concatenate([main[a : a + 1], main[b : b + 1], rest[a : a + 1], rest[b : b + 1]], axis=1))
    return rows


def decoded(rows, core):
    main = jnp.concatenate([r[:, k * LANE : (k + 1) * LANE] for r in rows for k in range(PAIR)], axis=0)
    rest = jnp.concatenate(
        [r[:, PAIR * LANE + k * REST : PAIR * LANE + (k + 1) * REST] for r in rows for k in range(PAIR)], axis=0
    )
    return jnp.where(
        core == 0, jnp.concatenate([main, rest], axis=1), jnp.concatenate([rest, main], axis=1)
    )


def copies_of(operator_ref, held, sems):
    width = operator_ref.shape[1] // COPIES

    def copy_of(k):
        columns = pl.ds(pl.multiple_of(k * width, LANE), width)
        return pltpu.make_async_copy(operator_ref.at[:, columns], held.at[:, columns], sems.at[k])

    return copy_of


def product(matrix, vector, lifted_ref, copy_of, held, spread, cut_ref, home):
    lifted = nt(vector, matrix)
    lifted_ref[...] = lifted
    turned = lifted.T
    for s in range(SYS):
        spread[s] = jnp.broadcast_to(turned[:, s : s + 1], (UNK, LANE))
    low = iota((1, LANE), 1) < REST

    def one(step, carry):
        totals = [[[None] * TILES for _ in range(SYS)] for _ in range(TOGETHER)]
        base = pl.multiple_of(step * (TOGETHER * NC * UNK), LANE)
        for j in range(UNK // 8):
            for s in range(SYS):
                v = spread[s, 8 * j : 8 * j + 8, :]
                for g in range(TOGETHER):
                    for k in range(TILES):
                        term = held[8 * j : 8 * j + 8, pl.ds(base + (g * TILES + k) * LANE, LANE)] * v
                        totals[g][s][k] = term if j == 0 else totals[g][s][k] + term
        for g in range(TOGETHER):
            z = step * TOGETHER + g
            sums = [[jnp.sum(totals[g][s][k], axis=0, keepdims=True) for k in range(TILES)] for s in range(SYS)]
            for p in range(PAIRS):
                a, b = sums[PAIR * p], sums[PAIR * p + 1]
                lo = jnp.where(low, a[1], pltpu.roll(b[1], REST, 1))
                hi = jnp.where(low, pltpu.roll(a[1], REST, 1), b[1])
                for c, row in ((0, (a[0], b[0], lo)), (1, (a[2], b[2], hi))):
                    for k in range(TILES):
                        cut_ref[*home(p, z, c), :, k * LANE : (k + 1) * LANE] = row[k]
        return carry

    if copy_of is None:
        lax.fori_loop(0, NZ // TOGETHER, one, 0)
        return
    per = NZ // COPIES // TOGETHER

    def chunk(k, carry):
        copy_of(k).wait()
        return lax.fori_loop(k * per, (k + 1) * per, one, carry)

    lax.fori_loop(0, COPIES, chunk, 0)


def first_kernel(
    len_hbm, inverse_hbm, residual_hbm, iterate_hbm, operator_hbm,
    cut_ref, matrix_ref, lifted_ref, residual_ref, iterate_ref, held,
    spread, sems, lengths, inverse, small_sems,
):
    small = [
        pltpu.make_async_copy(source, target, small_sems.at[k])
        for k, (source, target) in enumerate(
            ((len_hbm, lengths), (inverse_hbm, inverse), (residual_hbm, residual_ref), (iterate_hbm, iterate_ref))
        )
    ]
    for copy in small:
        copy.start()
    copy_of = copies_of(operator_hbm, held, sems)
    copy_of(0).start()
    for copy in small:
        copy.wait()
    for k in range(1, COPIES):
        copy_of(k).start()
    residual = residual_ref[...]
    matrix = preconditioner(lengths, inverse[...])
    product(matrix, residual, lifted_ref, copy_of, held, spread, cut_ref, lambda p, z, c: (z, c * (PAIRS) + p))
    matrix_ref[...] = matrix


def forward_kernel(arrived_ref, sent_ref):
    rows = jnp.sum(arrived_ref[...], axis=0)
    pairs = PAIRS
    for k in range(NX * NC * NY):
        c = k // NY % NC
        sent_ref[k] = rows[c * pairs : (c + 1) * pairs]


def second_kernel(
    arrived_ref, matrix_ref, residual_ref, held, cut_ref, mapped_ref, lifted_ref, spread
):
    core, x = lax.axis_index("c"), lax.axis_index("x")
    total = None
    for k in range(NX * NC):
        part = arrived_ref[k * NY + x]
        total = part if total is None else total + part
    mapped = decoded([total[p] for p in range(PAIRS)], core)
    matrix = matrix_ref[...]
    far = lax.div(lax.axis_index("zh"), NH // 2)

    def home(p, z, c):
        row = p * NH + lax.div(z, NL)
        x = lax.div(row, EACH)
        return (x * NL + lax.rem(z, NL)) * NC + lax.rem(c + far, NC), row - x * EACH

    product(matrix, mapped, lifted_ref, None, held, spread, cut_ref, home)
    step = lax.axis_index("zh")
    for e, vector in enumerate((mapped, residual_ref[...])):
        extra = encoded(vector, core)
        for to in range(NX):
            row = jnp.zeros((1, WIDE), f32)
            for p in range(PAIRS):
                at = p * NH + step - to * EACH
                row = jnp.where((at >= 0) & (at < EACH), extra[p], row)
            for k in range(NL * NC):
                cut_ref[to * NL * NC + k, EACH + e] = row
    mapped_ref[...] = mapped


def share_kernel(arrived_ref, sent_ref):
    near = jnp.sum(arrived_ref[:, :EACH], axis=0)
    own = (lax.axis_index("y") * NL + lax.axis_index("zl")) * NC + turned_core()
    rows = [near[j] for j in range(EACH)] + [arrived_ref[own, EACH], arrived_ref[own, EACH + 1]]
    for k in range(NH):
        for j, row in enumerate(rows):
            for i in range(TILES):
                sent_ref[k, j * TILES + i : j * TILES + i + 1, :] = row[:, i * LANE : (i + 1) * LANE]


def dots_kernel(far_ref, sent_ref):
    base = lax.axis_index("x") * EACH
    first = lax.div(base, NH)
    step = lax.axis_index("zh")
    mine = jnp.zeros((1, WIDE), f32)
    terms = [jnp.zeros((1, WIDE), f32)] * (2 * DOTS)
    total = far_ref[0]
    for k in range(1, NH):
        total = total + far_ref[k]

    def row(block, j):
        return jnp.concatenate([block[j * TILES + i : j * TILES + i + 1] for i in range(TILES)], axis=1)

    for j in range(EACH):
        t = row(total, j)
        h = lax.rem(base + j, NH)
        mine = jnp.where(h == step, t, mine)
        m, r = (
            jnp.concatenate([far_ref[h, k * TILES + i : k * TILES + i + 1, :] for i in range(TILES)], axis=1)
            for k in (EACH, EACH + 1)
        )
        same = lax.div(base + j, NH) == first
        for d, term in enumerate((r * r, r * m, m * m, t * r, t * m, t * t)):
            terms[d] = terms[d] + jnp.where(same, term, 0.0)
            terms[DOTS + d] = terms[DOTS + d] + jnp.where(same, 0.0, term)
    terms = jnp.concatenate(terms, axis=0)
    main, other, shared = (terms[:, k * LANE : (k + 1) * LANE] for k in range(TILES))
    low = iota(shared.shape, 1) < REST
    main = main + jnp.where(low, shared, 0.0)
    other = other + jnp.where(low, 0.0, shared)
    column = jnp.sum(
        jnp.concatenate([main[:DOTS], other[:DOTS], main[DOTS:], other[DOTS:]], axis=0), axis=1, keepdims=True
    )
    shape = (2 * PAIR * DOTS, LANE)
    place = iota(shape, 0) + first * (PAIR * DOTS)
    line = jnp.sum(jnp.where(place == iota(shape, 1), column, 0.0), axis=0, keepdims=True)
    sent = jnp.concatenate([mine, line], axis=1)
    for k in range(sent_ref.shape[0]):
        sent_ref[k] = sent


def last_kernel(arrived_ref, iterate_ref, residual_ref, mapped_ref, lifted_ref, lifted_two_ref, new_iterate_ref, new_residual_ref):
    core, x = lax.axis_index("c"), lax.axis_index("x")
    totals = jnp.sum(arrived_ref[:, :, WIDE:], axis=0)
    lane = iota((SYS, LANE), 1)
    system = iota((SYS, LANE), 0)
    home = (system // PAIR) * (PAIR * DOTS) + (system % PAIR) * DOTS
    norm_res, curve_one, square_map, mixed_res, mixed_map, square_two = (
        jnp.sum(jnp.where(lane == home + d, totals, 0.0), axis=1, keepdims=True) for d in range(DOTS)
    )
    alpha = norm_res / curve_one
    cross_mid = curve_one - alpha * square_map - alpha * mixed_res + alpha * alpha * mixed_map
    square_mid = square_map - 2.0 * alpha * mixed_map + alpha * alpha * square_two
    omega = cross_mid / square_mid
    mapped, lifted = mapped_ref[...], lifted_ref[...]
    rows = []
    for p in range(PAIRS):
        source = lax.div(p * NH + lax.axis_index("zh"), EACH)
        rows.append(arrived_ref[((source * NL + lax.axis_index("zl")) * NC + turned_core()) * NY + x][:, :WIDE])
    mapped_two = decoded(rows, core)
    middle = residual_ref[...] - alpha * mapped
    lifted_mid = lifted - alpha * lifted_two_ref[...]
    new_iterate_ref[...] = iterate_ref[...] + alpha * lifted + omega * lifted_mid
    new_residual_ref[...] = middle - omega * (mapped - alpha * mapped_two)


def exchanged(pieces, axes, groups=None):
    return lax.all_to_all(pieces, axes, split_axis=0, concat_axis=0, tiled=True, axis_index_groups=groups)


def crossed(length):
    return [[k * NC + (g + 2 * k // length) % NC for k in range(length)] for g in range(NC)]


def turned_core():
    return lax.rem(lax.axis_index("c") + lax.div(lax.axis_index("zh"), NH // 2), NC)


def body(operator, block_inverse, block_len, iterate, residual):
    def shape(*lengths):
        return jax.ShapeDtypeStruct(lengths, f32)

    hbm = pl.BlockSpec(memory_space=pltpu.HBM)
    small = shape(SYS, UNK)
    scratch = [pltpu.VMEM((SYS, UNK, LANE), f32)]
    params = pltpu.CompilerParams(vmem_limit_bytes=16 << 20)
    light = pltpu.CompilerParams(vmem_limit_bytes=4 << 20)
    inputs = (block_len, block_inverse.reshape(BLOCKS * BLOCKS, BLOCKS), residual, iterate, operator)
    inputs = [pltpu.with_memory_space_constraint(a, pltpu.HBM) for a in inputs]

    cut, matrix, lifted, residual, iterate, held = pl.pallas_call(
        first_kernel,
        out_shape=(shape(NZ, NC * PAIRS, 1, WIDE), shape(UNK, UNK), small, small, small, shape(*operator.shape)),
        in_specs=[hbm] * 5,
        out_specs=[VM] * 6,
        scratch_shapes=[
            *scratch,
            pltpu.SemaphoreType.DMA((COPIES,)),
            pltpu.SMEM((1, BLOCKS), jnp.int32),
            pltpu.VMEM((BLOCKS * BLOCKS, BLOCKS), f32),
            pltpu.SemaphoreType.DMA((4,)),
        ],
        compiler_params=params,
        name="first_product",
    )(*inputs)

    def call(kernel, name, out_shape, *operands):
        return pl.pallas_call(
            kernel,
            out_shape=out_shape,
            in_specs=[VM] * len(operands),
            out_specs=jax.tree.map(lambda _: VM, out_shape),
            compiler_params=light,
            name=name,
        )(*operands)

    sent = call(forward_kernel, "forward", shape(NX * NC * NY, PAIRS, 1, WIDE), exchanged(cut, Z))
    arrived = exchanged(sent, ("x", "c", "y"))

    cut, mapped, lifted_two = pl.pallas_call(
        second_kernel,
        out_shape=(shape(NX * NL * NC, EACH + 2, 1, WIDE), small, small),
        in_specs=[VM] * 4,
        out_specs=[VM] * 3,
        scratch_shapes=scratch,
        compiler_params=params,
        name="second_product",
    )(arrived, matrix, residual, held)

    sent = call(share_kernel, "share", shape(NH, (EACH + 2) * TILES, LANE), exchanged(cut, ("x", "zl", "c")))
    sent = call(dots_kernel, "dots", shape(NX * NL * NC * NY, 1, WIDE + LANE), exchanged(sent, ("zh", "c"), crossed(NH)))
    arrived = exchanged(sent, ("x", "zl", "c", "y"))
    return call(last_kernel, "update", (small, small), arrived, iterate, residual, mapped, lifted, lifted_two)


def solution(mesh):
    torus = Mesh(mesh.devices.reshape(NX, NH, NL, NC, NY), (*ROWS, "y"))
    placed = (P(ROWS, "y"), P(ROWS, None, None), P(ROWS, None), P(None, ROWS), P(None, ROWS))
    return jax.shard_map(
        body, mesh=torus, in_specs=placed, out_specs=(P(None, ROWS), P(None, ROWS)), check_vma=False
    )
```
